32 devices in a mesh: dp: 1 (over z), x: 4 (over y), y: 8 (over x, core).
Axes of the slice: x: 4, y: 4, z: 1, core: 2. Of those that a mesh axis runs over, the one named last changes fastest.
The devices are a block of a 4x4x8 slice.
Arguments:
- hidden: bfloat16 [1024, 1024], P('dp', 'x')
- w_qkv: bfloat16 [1024, 3072], P('x', 'y')
- b_qkv: bfloat16 [3072], P('y')
- w_out: bfloat16 [1024, 1024], P('y', 'x')
- b_out: bfloat16 [1024], P('x')
- attn_gain: bfloat16 [1024], P('x')
- attn_shift: bfloat16 [1024], P('x')
- w_up: bfloat16 [1024, 2, 4096], P('x', None, 'y')
- b_up: bfloat16 [2, 4096], P(None, 'y')
- w_down: bfloat16 [4096, 1024], P('y', 'x')
- b_down: bfloat16 [1024], P('x')
- mlp_gain: bfloat16 [1024], P('x')
- mlp_shift: bfloat16 [1024], P('x')
- k_cache: bfloat16 [1024, 64, 16, 64], P('dp', None, 'y')
- v_cache: bfloat16 [1024, 64, 16, 64], P('dp', None, 'y')
- positions: int32 [1024], P('dp')
- lengths: int32 [1024], P('dp')
Outputs:
- output 1: bfloat16 [1024, 1024], P('dp', 'x')
- output 2: bfloat16 [1024, 64, 16, 64], P('dp', None, 'y')
- output 3: bfloat16 [1024, 64, 16, 64], P('dp', None, 'y')
All inputs are finite; a program needn't handle non-finite values.
Results may differ from the reference program's by a relative error of at most 0.02.
Values are sent between devices in bfloat16 or wider.
A program may use at most 768 MiB of HBM per device.

```python
import math
import jax
import jax.numpy as jnp
from jax import lax

D = 1024
HEADS = 16
HEAD = 64
FF = 4096
BATCH_ROWS = 1024
CACHE_LEN = 64

DEEP_ALPHA = math.sqrt(140.0)
LN_EPS = 1e-5
ROPE_BASE = 10000.0


def setup_inputs(seed: int = 0, part: int = 0) -> dict:
    root_key = jax.random.key(seed)
    weight_keys = jax.random.split(root_key, 12)
    part_keys = jax.random.split(jax.random.fold_in(root_key, part), 5)

    def draw_normal(key, shape, scale):
        return jax.random.normal(key, shape, jnp.float32) * scale

    col_ramp = 0.4 + 1.2 * jnp.arange(D, dtype=jnp.float32) / D
    hidden = (draw_normal(part_keys[0], (BATCH_ROWS, D), 1.0) * col_ramp).astype(jnp.bfloat16)
    w_qkv = draw_normal(weight_keys[0], (D, 3 * D), D ** -0.5).astype(jnp.bfloat16)
    b_qkv = draw_normal(weight_keys[1], (3 * D,), 0.5).astype(jnp.bfloat16)
    w_out = draw_normal(weight_keys[2], (D, D), 2.0 * DEEP_ALPHA * D ** -0.5).astype(jnp.bfloat16)
    b_out = draw_normal(weight_keys[3], (D,), 0.3 * DEEP_ALPHA).astype(jnp.bfloat16)
    attn_gain = (col_ramp * (1.0 + draw_normal(weight_keys[4], (D,), 0.2))).astype(jnp.bfloat16)
    attn_shift = draw_normal(weight_keys[5], (D,), 0.3).astype(jnp.bfloat16)
    w_up = draw_normal(weight_keys[6], (D, 2, FF), D ** -0.5).astype(jnp.bfloat16)
    b_up = draw_normal(weight_keys[7], (2, FF), 0.5).astype(jnp.bfloat16)
    w_down = draw_normal(weight_keys[8], (FF, D), 1.2 * DEEP_ALPHA * FF ** -0.5).astype(jnp.bfloat16)
    b_down = draw_normal(weight_keys[9], (D,), 0.3 * DEEP_ALPHA).astype(jnp.bfloat16)
    mlp_gain = (1.0 + draw_normal(weight_keys[10], (D,), 0.3)).astype(jnp.bfloat16)
    mlp_shift = draw_normal(weight_keys[11], (D,), 0.3).astype(jnp.bfloat16)
    k_cache = draw_normal(part_keys[1], (BATCH_ROWS, CACHE_LEN, HEADS, HEAD), 2.0).astype(jnp.bfloat16)
    v_cache = draw_normal(part_keys[2], (BATCH_ROWS, CACHE_LEN, HEADS, HEAD), 1.0).astype(jnp.bfloat16)
    lengths = jax.random.randint(part_keys[3], (BATCH_ROWS,), 0, CACHE_LEN, jnp.int32)
    lengths = lengths.at[0].set(CACHE_LEN - 1).at[1].set(0)
    offsets = jax.random.randint(part_keys[4], (BATCH_ROWS,), 0, CACHE_LEN, jnp.int32)
    offsets = offsets.at[2].set(CACHE_LEN - 1).at[3].set(0)
    positions = lengths + offsets
    return {'hidden': hidden, 'w_qkv': w_qkv, 'b_qkv': b_qkv, 'w_out': w_out, 'b_out': b_out, 'attn_gain': attn_gain, 'attn_shift': attn_shift, 'w_up': w_up, 'b_up': b_up, 'w_down': w_down, 'b_down': b_down, 'mlp_gain': mlp_gain, 'mlp_shift': mlp_shift, 'k_cache': k_cache, 'v_cache': v_cache, 'positions': positions, 'lengths': lengths}


def apply_rotary(head_vec, positions):
    half_dim = HEAD // 2
    inv_freq = ROPE_BASE ** (-2.0 * jnp.arange(half_dim, dtype=jnp.float32) / HEAD)
    angles = positions.astype(jnp.float32)[:, None] * inv_freq[None, :]
    cos_table = jnp.cos(angles)[:, None, :]
    sin_table = jnp.sin(angles)[:, None, :]
    vec_wide = head_vec.astype(jnp.float32)
    lower_half = vec_wide[..., :half_dim]
    upper_half = vec_wide[..., half_dim:]
    return jnp.concatenate([lower_half * cos_table - upper_half * sin_table, upper_half * cos_table + lower_half * sin_table], axis=-1).astype(jnp.bfloat16)


def layer_norm(h_val, gain, shift):
    mean_row = jnp.mean(h_val, axis=-1, keepdims=True)
    var_row = jnp.mean(jnp.square(h_val - mean_row), axis=-1, keepdims=True)
    return (h_val - mean_row) * lax.rsqrt(var_row + LN_EPS) * gain.astype(jnp.float32) + shift.astype(jnp.float32)


def reference(hidden, w_qkv, b_qkv, w_out, b_out, attn_gain, attn_shift, w_up, b_up, w_down, b_down, mlp_gain, mlp_shift, k_cache, v_cache, positions, lengths):
    qkv_vals = (jnp.dot(hidden, w_qkv, preferred_element_type=jnp.float32) + b_qkv.astype(jnp.float32)).astype(jnp.bfloat16)
    qkv_vals = qkv_vals.reshape(BATCH_ROWS, HEADS, 3, HEAD)
    query_rot = apply_rotary(qkv_vals[:, :, 0], positions)
    key_rot = apply_rotary(qkv_vals[:, :, 1], positions)
    slot_hit = (jnp.arange(CACHE_LEN)[None, :] == lengths[:, None])[:, :, None, None]
    k_full = jnp.where(slot_hit, key_rot[:, None], k_cache)
    v_full = jnp.where(slot_hit, qkv_vals[:, None, :, 2], v_cache)

    def attend_row(row_args):
        query_row, key_row, value_row, length_row = row_args
        scores = jnp.einsum('hd,shd->hs', query_row.astype(jnp.float32), key_row.astype(jnp.float32)) * (HEAD ** -0.5)
        slot_ok = jnp.arange(CACHE_LEN)[None, :] <= length_row
        scores = jnp.where(slot_ok, scores, -1e30)
        attn_probs = jax.nn.softmax(scores, axis=-1).astype(jnp.bfloat16).astype(jnp.float32)
        return jnp.einsum('hs,shd->hd', attn_probs, value_row.astype(jnp.float32)).astype(jnp.bfloat16)

    attn_out = lax.map(attend_row, (query_rot, k_full, v_full, lengths)).reshape(BATCH_ROWS, D)
    proj_sum = jnp.dot(attn_out, w_out, preferred_element_type=jnp.float32) + b_out.astype(jnp.float32)
    h_attn = DEEP_ALPHA * hidden.astype(jnp.float32) + proj_sum
    normed = layer_norm(h_attn, attn_gain, attn_shift).astype(jnp.bfloat16)
    up_sum = jnp.dot(normed, w_up.reshape(D, 2 * FF), preferred_element_type=jnp.float32).reshape(BATCH_ROWS, 2, FF) + b_up.astype(jnp.float32)
    gated_act = (jax.nn.gelu(up_sum[:, 0], approximate=True) * up_sum[:, 1]).astype(jnp.bfloat16)
    down_sum = jnp.dot(gated_act, w_down, preferred_element_type=jnp.float32)
    h_mlp = DEEP_ALPHA * normed.astype(jnp.float32) + down_sum + b_down.astype(jnp.float32)
    result = layer_norm(h_mlp, mlp_gain, mlp_shift).astype(jnp.bfloat16)
    return (result, k_full, v_full)
```

```python
import functools
import math
import jax
import jax.numpy as jnp
from jax import lax
from jax.experimental import pallas as pl
from jax.experimental.pallas import tpu as pltpu
from jax.sharding import PartitionSpec as P

DEEP_ALPHA = math.sqrt(140.0)
LN_EPS = 1e-5
ROPE_BASE = 10000.0
MESH = pl.DeviceIdType.MESH
CORES = 2
F32 = jnp.float32
BF16 = jnp.bfloat16


def layer_norm(h_val, gain, shift):
    mean_row = jnp.mean(h_val, axis=-1, keepdims=True)
    cent = h_val - mean_row
    var_row = jnp.mean(cent * cent, axis=-1, keepdims=True)
    return (cent * lax.rsqrt(var_row + LN_EPS) * gain + shift).astype(BF16)


def tail_kernel(nx, ny, attn_ref, hid_ref, wo_ref, vec_ref, wup_ref, bup_ref, wdn_ref, out_ref,
                part1, dbuf1, sbuf1, rbuf1, part2, dbuf2, sbuf2, rbuf2, zall, obuf, send, recv):
    nc = ny // CORES
    x, y = lax.axis_index('x'), lax.axis_index('y')
    core, chip = lax.rem(y, CORES), lax.div(y, CORES)
    partner = {'y': chip * CORES + (1 - core)}
    blk = core * nc + chip
    rows = hid_ref.shape[0]
    width = vec_ref.shape[2]

    def chip_at(d):
        return lax.rem(chip + d + nc, nc)

    def x_at(d):
        return lax.rem(x + d + nx, nx)

    def chip_dev(d):
        return {'y': chip_at(d) * CORES + core}

    def copy(src, dst, i, dev):
        return pltpu.make_async_remote_copy(src_ref=src, dst_ref=dst, send_sem=send.at[i], recv_sem=recv.at[i],
                                            device_id=dev, device_id_type=MESH)

    barrier = pltpu.get_barrier_semaphore()
    pl.semaphore_signal(barrier, inc=1, device_id=partner, device_id_type=MESH)
    for d in range(1, nc):
        pl.semaphore_signal(barrier, inc=1, device_id=chip_dev(d), device_id_type=MESH)
    for d in range(1, nx):
        pl.semaphore_signal(barrier, inc=1, device_id={'x': x_at(d)}, device_id_type=MESH)
    pl.semaphore_wait(barrier, nc + nx - 1)

    def vec(i):
        return jnp.concatenate([vec_ref[b, i:i + 1, :] for b in range(nx)], axis=1).astype(F32)

    def scatter_sum(part, dbuf, sbuf, rbuf, base):
        cp = copy(part.at[1 - core], dbuf, base, partner)
        cp.start()
        cp.wait()
        sbuf[...] = (part[core].astype(F32) + dbuf[...].astype(F32)).astype(BF16)
        cps = [copy(sbuf.at[chip_at(d)], rbuf.at[d - 1], base + d, chip_dev(d)) for d in range(1, nc)]
        for cp in cps:
            cp.start()
        total = sbuf[chip].astype(F32)
        for d in range(1, nc):
            cps[d - 1].wait()
            total = total + rbuf[d - 1].astype(F32)
        return total

    def share(buf_at, base):
        far = [copy(buf_at(blk), buf_at(blk), base + d - 1, chip_dev(d)) for d in range(1, nc)]
        for cp in far:
            cp.start()
        near = [copy(buf_at(blk), buf_at(blk), base + nc - 1, partner)]
        near[0].start()
        for d in range(1, nc):
            b = core * nc + chip_at(-d)
            copy(buf_at(b), buf_at(b), base + d - 1, chip_dev(d)).wait_recv()
            cp = copy(buf_at(b), buf_at(b), base + nc - 1 + d, partner)
            cp.start()
            near.append(cp)
        for d in range(nc):
            b = (1 - core) * nc + chip_at(-d)
            copy(buf_at(b), buf_at(b), base + nc - 1 + d, partner).wait_recv()
        for cp in far + near:
            cp.wait_send()

    per = 2 * nc - 1
    base1, base2, base3, base4, base5 = 0, nc, nc + per, 2 * nc + per, 2 * nc + per + nx

    for b in range(nx):
        res = jnp.dot(attn_ref[...], wo_ref[b], preferred_element_type=F32).astype(BF16)
        part1[:, :, :, b * width:(b + 1) * width] = res.reshape(CORES, nc, rows, width)
    total = scatter_sum(part1, dbuf1, sbuf1, rbuf1, base1)
    h_attn = DEEP_ALPHA * hid_ref[...].astype(F32) + total + vec(0)
    z_own = layer_norm(h_attn, vec(1), vec(2))
    zall[blk] = z_own
    share(lambda b: zall.at[b], base2)

    z = zall[...].reshape(ny * rows, nx * width)
    gate = bup_ref[0:1, :].astype(F32)
    val = bup_ref[1:2, :].astype(F32)
    for b in range(nx):
        zb = z[:, b * width:(b + 1) * width]
        gate = gate + jnp.dot(zb, wup_ref[b, 0], preferred_element_type=F32)
        val = val + jnp.dot(zb, wup_ref[b, 1], preferred_element_type=F32)
    g = (jax.nn.gelu(gate, approximate=True) * val).astype(BF16)
    for b in range(nx):
        res = jnp.dot(g, wdn_ref[b], preferred_element_type=F32).astype(BF16)
        part2[:, :, :, b * width:(b + 1) * width] = res.reshape(CORES, nc, rows, width)
    total = scatter_sum(part2, dbuf2, sbuf2, rbuf2, base3)
    h_mlp = DEEP_ALPHA * zall[blk].astype(F32) + total + vec(3)
    o = layer_norm(h_mlp, vec(4), vec(5))
    for b in range(nx):
        obuf[b] = o[:, b * width:(b + 1) * width]
    cps = [copy(obuf.at[x_at(d)], out_ref.at[x, blk], base4 + d, {'x': x_at(d)}) for d in range(1, nx)]
    for cp in cps:
        cp.start()
    out_ref[x, blk] = obuf[x]
    for d in range(1, nx):
        copy(obuf.at[x_at(d)], out_ref.at[x_at(-d), blk], base4 + d, {'x': x_at(d)}).wait_recv()
    share(lambda b: out_ref.at[:, b], base5)
    for cp in cps:
        cp.wait_send()


def tail(nx, ny, attn, hid, wo, vecs, wup, bup, wdn):
    nc = ny // CORES
    rows, total_width = hid.shape
    width = total_width // nx
    n_sem = 2 * nc + 2 * (2 * nc - 1) + nx + 1
    vm = pl.BlockSpec(memory_space=pltpu.VMEM)
    reduce_bufs = [pltpu.VMEM((CORES, nc, rows, total_width), BF16), pltpu.VMEM((nc, rows, total_width), BF16),
                   pltpu.VMEM((nc, rows, total_width), BF16), pltpu.VMEM((nc - 1, rows, total_width), BF16)]
    out = pl.pallas_call(
        functools.partial(tail_kernel, nx, ny),
        out_shape=jax.ShapeDtypeStruct((nx, ny, rows, width), BF16),
        in_specs=[vm] * 7,
        out_specs=vm,
        scratch_shapes=reduce_bufs + reduce_bufs + [
            pltpu.VMEM((ny, rows, total_width), BF16), pltpu.VMEM((nx, rows, width), BF16),
            pltpu.SemaphoreType.DMA((n_sem,)), pltpu.SemaphoreType.DMA((n_sem,))],
        compiler_params=pltpu.CompilerParams(collective_id=0, has_side_effects=True),
        name='tail',
    )(attn, hid, wo, vecs, wup, bup, wdn)
    return out.reshape(nx * ny * rows, width)


def apply_rotary(head_vec, positions):
    head_dim = head_vec.shape[-1]
    half_dim = head_dim // 2
    inv_freq = ROPE_BASE ** (-2.0 * jnp.arange(half_dim, dtype=jnp.float32) / head_dim)
    angles = positions.astype(jnp.float32)[:, None] * inv_freq[None, :]
    cos_table = jnp.cos(angles)[:, None, :]
    sin_table = jnp.sin(angles)[:, None, :]
    vec_wide = head_vec.astype(jnp.float32)
    lower_half = vec_wide[..., :half_dim]
    upper_half = vec_wide[..., half_dim:]
    return jnp.concatenate([lower_half * cos_table - upper_half * sin_table, upper_half * cos_table + lower_half * sin_table], axis=-1).astype(jnp.bfloat16)


def write_slot(cache, new_rows, lengths):
    slot_hit = jnp.arange(cache.shape[1])[None, :, None, None] == lengths[:, None, None, None]
    return jnp.where(slot_hit, new_rows[:, None], cache)


def attend(query_rot, k_full, v_full, lengths):
    head_dim = query_rot.shape[-1]
    scores = jnp.einsum('bhd,bshd->bhs', query_rot, k_full, preferred_element_type=jnp.float32) * (head_dim ** -0.5)
    slot_ok = jnp.arange(k_full.shape[1])[None, None, :] <= lengths[:, None, None]
    scores = jnp.where(slot_ok, scores, -1e30)
    attn_probs = jax.nn.softmax(scores, axis=-1).astype(jnp.bfloat16)
    attn_mixed = jnp.einsum('bhs,bshd->bhd', attn_probs, v_full, preferred_element_type=jnp.float32)
    return attn_mixed.astype(jnp.bfloat16).reshape(query_rot.shape[0], -1)


def solution(mesh):
    nx, ny = mesh.shape['x'], mesh.shape['y']
    cache_spec = P('dp', None, 'y', None)
    width_spec = P('x')
    in_specs = (P('dp', 'x'), P('x', 'y'), P('y'), P('y', 'x'), width_spec, width_spec, width_spec, P('x', None, 'y'), P(None, 'y'), P('y', 'x'), width_spec, width_spec, width_spec, cache_spec, cache_spec, P('dp'), P('dp'))
    out_specs = (P('dp', 'x'), cache_spec, cache_spec)

    def local_step(hidden, w_qkv, b_qkv, w_out, b_out, attn_gain, attn_shift, w_up, b_up, w_down, b_down, mlp_gain, mlp_shift, k_cache, v_cache, positions, lengths):
        row_count, width_local = hidden.shape
        local_heads, head_dim = k_cache.shape[2], k_cache.shape[3]
        x, y = lax.axis_index('x'), lax.axis_index('y')
        hidden_all = lax.all_gather(hidden, 'x', axis=1, tiled=True)
        wqkv_all = lax.all_gather(w_qkv, 'x', axis=0, tiled=True)
        vecs = jnp.stack([b_out, attn_gain, attn_shift, b_down, mlp_gain, mlp_shift, b_out, b_out])
        vecs = lax.all_gather(vecs, 'x')
        wo = lax.all_gather(w_out, 'x')
        wup = lax.all_gather(jnp.transpose(w_up, (1, 0, 2)), 'x')
        wdn = lax.all_gather(w_down, 'x')
        qkv_vals = (jnp.dot(hidden_all, wqkv_all, preferred_element_type=jnp.float32) + b_qkv.astype(jnp.float32)).astype(jnp.bfloat16)
        qkv_vals = qkv_vals.reshape(row_count, local_heads, 3, head_dim)
        query_rot = apply_rotary(qkv_vals[:, :, 0], positions)
        k_full = write_slot(k_cache, apply_rotary(qkv_vals[:, :, 1], positions), lengths)
        v_full = write_slot(v_cache, qkv_vals[:, :, 2], lengths)
        attn_out = attend(query_rot, k_full, v_full, lengths)
        per_x = row_count // nx
        per = per_x // ny
        blk = lax.rem(y, CORES) * (ny // CORES) + lax.div(y, CORES)
        attn_own = lax.dynamic_slice_in_dim(attn_out, x * per_x, per_x, 0)
        hid_own = lax.dynamic_slice_in_dim(hidden_all, x * per_x + blk * per, per, 0)
        result = tail(nx, ny, attn_own, hid_own, wo, vecs, wup, b_up, wdn)
        return result, k_full, v_full

    return jax.shard_map(local_step, mesh=mesh, in_specs=in_specs, out_specs=out_specs, check_vma=False)
```

```python
import functools
import math
import jax
import jax.numpy as jnp
from jax import lax
from jax.experimental import pallas as pl
from jax.experimental.pallas import tpu as pltpu
from jax.sharding import PartitionSpec as P

DEEP_ALPHA = math.sqrt(140.0)
LN_EPS = 1e-5
ROPE_BASE = 10000.0
MESH = pl.DeviceIdType.MESH
CORES = 2
F32 = jnp.float32
BF16 = jnp.bfloat16


def layer_norm(h_val, gain, shift):
    mean_row = jnp.mean(h_val, axis=-1, keepdims=True)
    cent = h_val - mean_row
    var_row = jnp.mean(cent * cent, axis=-1, keepdims=True)
    return (cent * lax.rsqrt(var_row + LN_EPS) * gain + shift).astype(BF16)


def tail_kernel(nx, ny, attn_ref, hid_ref, wo_ref, vec_ref, wup_ref, bup_ref, wdn_ref, out_ref,
                part1, dbuf1, sbuf1, rbuf1, part2, dbuf2, sbuf2, rbuf2, zall, obuf, send, recv):
    nc = ny // CORES
    x, y = lax.axis_index('x'), lax.axis_index('y')
    core, chip = lax.rem(y, CORES), lax.div(y, CORES)
    partner = {'y': chip * CORES + (1 - core)}
    blk = core * nc + chip
    rows = hid_ref.shape[0]
    width = vec_ref.shape[2]

    def chip_at(d):
        return lax.rem(chip + d + nc, nc)

    def x_at(d):
        return lax.rem(x + d + nx, nx)

    def chip_dev(d):
        return {'y': chip_at(d) * CORES + core}

    def copy(src, dst, i, dev):
        return pltpu.make_async_remote_copy(src_ref=src, dst_ref=dst, send_sem=send.at[i], recv_sem=recv.at[i],
                                            device_id=dev, device_id_type=MESH)

    barrier = pltpu.get_barrier_semaphore()
    pl.semaphore_signal(barrier, inc=1, device_id=partner, device_id_type=MESH)
    for d in range(1, nc):
        pl.semaphore_signal(barrier, inc=1, device_id=chip_dev(d), device_id_type=MESH)
    for d in range(1, nx):
        pl.semaphore_signal(barrier, inc=1, device_id={'x': x_at(d)}, device_id_type=MESH)
    pl.semaphore_wait(barrier, nc + nx - 1)

    def vec(i):
        return jnp.concatenate([vec_ref[b, i:i + 1, :] for b in range(nx)], axis=1).astype(F32)

    def scatter_sum(part, dbuf, sbuf, rbuf, base):
        cp = copy(part.at[1 - core], dbuf, base, partner)
        cp.start()
        cp.wait()
        sbuf[...] = (part[core].astype(F32) + dbuf[...].astype(F32)).astype(BF16)
        cps = [copy(sbuf.at[chip_at(d)], rbuf.at[d - 1], base + d, chip_dev(d)) for d in range(1, nc)]
        for cp in cps:
            cp.start()
        total = sbuf[chip].astype(F32)
        for d in range(1, nc):
            cps[d - 1].wait()
            total = total + rbuf[d - 1].astype(F32)
        return total

    def share(buf_at, base):
        far = [copy(buf_at(blk), buf_at(blk), base + d - 1, chip_dev(d)) for d in range(1, nc)]
        for cp in far:
            cp.start()
        near = [copy(buf_at(blk), buf_at(blk), base + nc - 1, partner)]
        near[0].start()
        for d in range(1, nc):
            b = core * nc + chip_at(-d)
            copy(buf_at(b), buf_at(b), base + d - 1, chip_dev(d)).wait_recv()
            cp = copy(buf_at(b), buf_at(b), base + nc - 1 + d, partner)
            cp.start()
            near.append(cp)
        for d in range(nc):
            b = (1 - core) * nc + chip_at(-d)
            copy(buf_at(b), buf_at(b), base + nc - 1 + d, partner).wait_recv()
        for cp in far + near:
            cp.wait_send()

    per = 2 * nc - 1
    base1, base2, base3, base4, base5 = 0, nc, nc + per, 2 * nc + per, 2 * nc + per + nx

    for b in range(nx):
        res = jnp.dot(attn_ref[...], wo_ref[b], preferred_element_type=F32).astype(BF16)
        part1[:, :, :, b * width:(b + 1) * width] = res.reshape(CORES, nc, rows, width)
    total = scatter_sum(part1, dbuf1, sbuf1, rbuf1, base1)
    h_attn = DEEP_ALPHA * hid_ref[...].astype(F32) + total + vec(0)
    z_own = layer_norm(h_attn, vec(1), vec(2))
    zall[blk] = z_own
    share(lambda b: zall.at[b], base2)

    z = zall[...].reshape(ny * rows, nx * width)
    gate = bup_ref[0:1, :].astype(F32)
    val = bup_ref[1:2, :].astype(F32)
    for b in range(nx):
        zb = z[:, b * width:(b + 1) * width]
        gate = gate + jnp.dot(zb, wup_ref[b, 0], preferred_element_type=F32)
        val = val + jnp.dot(zb, wup_ref[b, 1], preferred_element_type=F32)
    g = (jax.nn.gelu(gate, approximate=True) * val).astype(BF16)
    for b in range(nx):
        res = jnp.dot(g, wdn_ref[b], preferred_element_type=F32).astype(BF16)
        part2[:, :, :, b * width:(b + 1) * width] = res.reshape(CORES, nc, rows, width)
    total = scatter_sum(part2, dbuf2, sbuf2, rbuf2, base3)
    h_mlp = DEEP_ALPHA * zall[blk].astype(F32) + total + vec(3)
    o = layer_norm(h_mlp, vec(4), vec(5))
    for b in range(nx):
        obuf[b] = o[:, b * width:(b + 1) * width]
    cps = [copy(obuf.at[x_at(d)], out_ref.at[x, blk], base4 + d, {'x': x_at(d)}) for d in range(1, nx)]
    for cp in cps:
        cp.start()
    out_ref[x, blk] = obuf[x]
    for d in range(1, nx):
        copy(obuf.at[x_at(d)], out_ref.at[x_at(-d), blk], base4 + d, {'x': x_at(d)}).wait_recv()
    share(lambda b: out_ref.at[:, b], base5)
    for cp in cps:
        cp.wait_send()


def tail(nx, ny, attn, hid, wo, vecs, wup, bup, wdn):
    nc = ny // CORES
    rows, total_width = hid.shape
    width = total_width // nx
    n_sem = 2 * nc + 2 * (2 * nc - 1) + nx + 1
    vm = pl.BlockSpec(memory_space=pltpu.VMEM)
    reduce_bufs = [pltpu.VMEM((CORES, nc, rows, total_width), BF16), pltpu.VMEM((nc, rows, total_width), BF16),
                   pltpu.VMEM((nc, rows, total_width), BF16), pltpu.VMEM((nc - 1, rows, total_width), BF16)]
    out = pl.pallas_call(
        functools.partial(tail_kernel, nx, ny),
        out_shape=jax.ShapeDtypeStruct((nx, ny, rows, width), BF16),
        in_specs=[vm] * 7,
        out_specs=vm,
        scratch_shapes=reduce_bufs + reduce_bufs + [
            pltpu.VMEM((ny, rows, total_width), BF16), pltpu.VMEM((nx, rows, width), BF16),
            pltpu.SemaphoreType.DMA((n_sem,)), pltpu.SemaphoreType.DMA((n_sem,))],
        compiler_params=pltpu.CompilerParams(collective_id=0, has_side_effects=True),
        name='tail',
    )(attn, hid, wo, vecs, wup, bup, wdn)
    return out.reshape(nx * ny * rows, width)


def cache_kernel(n_blocks, k_ref, v_ref, kn_ref, vn_ref, q_ref, lens_ref, lane_ref, ko_ref, vo_ref, attn_ref,
                 qs, sc, acc):
    step = pl.program_id(0)
    slots, heads, dim, _ = k_ref.shape
    own = q_ref.shape[2]
    cols = pl.ds(pl.multiple_of(lax.axis_index('x') * own, own), own)
    total_slots = n_blocks * slots

    @pl.when(step == 0)
    def _():
        qs[...] = q_ref[...].astype(F32)
        acc[...] = jnp.zeros_like(acc)

    def write(src, new, dst, first):
        for s in range(slots):
            hit = lane_ref[...] == (first + s).astype(F32).astype(BF16)
            for h in range(heads):
                for t in range(dim // 16):
                    part = pl.ds(t * 16, 16)
                    dst[s, h, part, :] = jnp.where(hit, new[h, part, :], src[s, h, part, :])

    @pl.when(step < n_blocks)
    def _():
        first = step * slots
        write(k_ref, kn_ref, ko_ref, first)
        for s in range(slots):
            for h in range(heads):
                sc[h, pl.ds(first + s, 1), :] = jnp.sum(
                    ko_ref[s, h, :, cols].astype(F32) * qs[h], axis=0, keepdims=True)

    @pl.when(step == n_blocks - 1)
    def _():
        slot = lax.broadcasted_iota(jnp.int32, (total_slots, own), 0)
        ok = slot <= lens_ref[:, cols]
        for h in range(heads):
            s = jnp.where(ok, sc[h] * (dim ** -0.5), -1e30)
            e = jnp.exp(s - jnp.max(s, axis=0, keepdims=True))
            p = e / jnp.sum(e, axis=0, keepdims=True)
            sc[h] = p.astype(BF16).astype(F32)

    @pl.when(step >= n_blocks)
    def _():
        first = (step - n_blocks) * slots
        write(v_ref, vn_ref, vo_ref, first)
        for h in range(heads):
            a = acc[h]
            for s in range(slots):
                a = a + vo_ref[s, h, :, cols].astype(F32) * sc[h, pl.ds(first + s, 1), :]
            acc[h] = a

    @pl.when(step == 2 * n_blocks - 1)
    def _():
        attn_ref[...] = acc[...].reshape(heads * dim, own).T.astype(BF16)


def cache_step(k_t, v_t, k_new, v_new, q_own, lengths, slots=4):
    total_slots, heads, dim, rows = k_t.shape
    own = q_own.shape[2]
    n = total_slots // slots
    blk = (slots, heads, dim, rows)
    lens = lengths.reshape(1, rows)
    lane = jnp.broadcast_to(lengths.astype(BF16)[None], (16, rows))
    k_spec = pl.BlockSpec(blk, lambda i: (jnp.minimum(i, n - 1), 0, 0, 0))
    v_spec = pl.BlockSpec(blk, lambda i: (jnp.maximum(i - n, 0), 0, 0, 0))
    whole = pl.BlockSpec(memory_space=pltpu.VMEM)
    shape = jax.ShapeDtypeStruct(k_t.shape, k_t.dtype)
    size = 4 * k_t.size * 2
    return pl.pallas_call(
        functools.partial(cache_kernel, n),
        grid=(2 * n,),
        out_shape=(shape, shape, jax.ShapeDtypeStruct((own, heads * dim), BF16)),
        in_specs=[k_spec, v_spec] + [whole] * 5,
        out_specs=(k_spec, v_spec, whole),
        scratch_shapes=[pltpu.VMEM((heads, dim, own), F32), pltpu.VMEM((heads, total_slots, own), F32),
                        pltpu.VMEM((heads, dim, own), F32)],
        cost_estimate=pl.CostEstimate(flops=40 * k_t.size, bytes_accessed=size, transcendentals=0),
        name='cache_step',
    )(k_t, v_t, k_new, v_new, q_own, lens, lane)


def apply_rotary(head_vec, positions):
    head_dim = head_vec.shape[-1]
    half_dim = head_dim // 2
    inv_freq = ROPE_BASE ** (-2.0 * jnp.arange(half_dim, dtype=jnp.float32) / head_dim)
    angles = positions.astype(jnp.float32)[:, None] * inv_freq[None, :]
    cos_table = jnp.cos(angles)[:, None, :]
    sin_table = jnp.sin(angles)[:, None, :]
    vec_wide = head_vec.astype(jnp.float32)
    lower_half = vec_wide[..., :half_dim]
    upper_half = vec_wide[..., half_dim:]
    return jnp.concatenate([lower_half * cos_table - upper_half * sin_table, upper_half * cos_table + lower_half * sin_table], axis=-1).astype(jnp.bfloat16)


def solution(mesh):
    nx, ny = mesh.shape['x'], mesh.shape['y']
    cache_spec = P('dp', None, 'y', None)
    width_spec = P('x')
    in_specs = (P('dp', 'x'), P('x', 'y'), P('y'), P('y', 'x'), width_spec, width_spec, width_spec, P('x', None, 'y'), P(None, 'y'), P('y', 'x'), width_spec, width_spec, width_spec, cache_spec, cache_spec, P('dp'), P('dp'))
    out_specs = (P('dp', 'x'), cache_spec, cache_spec)

    def local_step(hidden, w_qkv, b_qkv, w_out, b_out, attn_gain, attn_shift, w_up, b_up, w_down, b_down, mlp_gain, mlp_shift, k_cache, v_cache, positions, lengths):
        row_count, width_local = hidden.shape
        local_heads, head_dim = k_cache.shape[2], k_cache.shape[3]
        x, y = lax.axis_index('x'), lax.axis_index('y')
        hidden_all = lax.all_gather(hidden, 'x', axis=1, tiled=True)
        wqkv_all = lax.all_gather(w_qkv, 'x', axis=0, tiled=True)
        vecs = jnp.stack([b_out, attn_gain, attn_shift, b_down, mlp_gain, mlp_shift, b_out, b_out])
        vecs = lax.all_gather(vecs, 'x')
        wo = lax.all_gather(w_out, 'x')
        wup = lax.all_gather(jnp.transpose(w_up, (1, 0, 2)), 'x')
        wdn = lax.all_gather(w_down, 'x')
        qkv_vals = (jnp.dot(hidden_all, wqkv_all, preferred_element_type=jnp.float32) + b_qkv.astype(jnp.float32)).astype(jnp.bfloat16)
        qkv_vals = qkv_vals.reshape(row_count, local_heads, 3, head_dim)
        heads_first = lambda v: jnp.transpose(v, (1, 2, 0))
        per_x = row_count // nx
        q_t = heads_first(apply_rotary(qkv_vals[:, :, 0], positions))
        q_own = lax.dynamic_slice_in_dim(q_t, x * per_x, per_x, 2)
        k_new = heads_first(apply_rotary(qkv_vals[:, :, 1], positions))
        v_new = heads_first(qkv_vals[:, :, 2])
        k_t, v_t = jnp.transpose(k_cache, (1, 2, 3, 0)), jnp.transpose(v_cache, (1, 2, 3, 0))
        k_t, v_t, attn_own = cache_step(k_t, v_t, k_new, v_new, q_own, lengths)
        k_full, v_full = jnp.transpose(k_t, (3, 0, 1, 2)), jnp.transpose(v_t, (3, 0, 1, 2))
        per = per_x // ny
        blk = lax.rem(y, CORES) * (ny // CORES) + lax.div(y, CORES)
        hid_own = lax.dynamic_slice_in_dim(hidden_all, x * per_x + blk * per, per, 0)
        result = tail(nx, ny, attn_own, hid_own, wo, vecs, wup, b_up, wdn)
        return result, k_full, v_full

    return jax.shard_map(local_step, mesh=mesh, in_specs=in_specs, out_specs=out_specs, check_vma=False)
```

```python
import functools
import math
import jax
import jax.numpy as jnp
from jax import lax
from jax.experimental import pallas as pl
from jax.experimental.pallas import tpu as pltpu
from jax.sharding import PartitionSpec as P

DEEP_ALPHA = math.sqrt(140.0)
LN_EPS = 1e-5
ROPE_BASE = 10000.0
MESH = pl.DeviceIdType.MESH
CORES = 2
F32 = jnp.float32
BF16 = jnp.bfloat16


def layer_norm(h_val, gain, shift):
    mean_row = jnp.mean(h_val, axis=-1, keepdims=True)
    cent = h_val - mean_row
    var_row = jnp.mean(cent * cent, axis=-1, keepdims=True)
    return (cent * lax.rsqrt(var_row + LN_EPS) * gain + shift).astype(BF16)


def tail_kernel(nx, ny, attn_ref, hid_ref, vec_ref, bup_ref, *refs):
    wo_ref, wup_ref, wdn_ref = refs[:nx], refs[nx:2 * nx], refs[2 * nx:3 * nx]
    (out_ref, part1, dbuf1, sbuf1, rbuf1, part2, dbuf2, sbuf2, rbuf2, zall, obuf, send, recv) = refs[3 * nx:]
    nc = ny // CORES
    x, y = lax.axis_index('x'), lax.axis_index('y')
    core, chip = lax.rem(y, CORES), lax.div(y, CORES)
    partner = {'y': chip * CORES + (1 - core)}
    blk = core * nc + chip
    rows = hid_ref.shape[0]
    width = hid_ref.shape[1] // nx

    def chip_at(d):
        return lax.rem(chip + d + nc, nc)

    def x_at(d):
        return lax.rem(x + d + nx, nx)

    def chip_dev(d):
        return {'y': chip_at(d) * CORES + core}

    def copy(src, dst, i, dev):
        return pltpu.make_async_remote_copy(src_ref=src, dst_ref=dst, send_sem=send.at[i], recv_sem=recv.at[i],
                                            device_id=dev, device_id_type=MESH)

    barrier = pltpu.get_barrier_semaphore()
    pl.semaphore_signal(barrier, inc=1, device_id=partner, device_id_type=MESH)
    for d in range(1, nc):
        pl.semaphore_signal(barrier, inc=1, device_id=chip_dev(d), device_id_type=MESH)
    for d in range(1, nx):
        pl.semaphore_signal(barrier, inc=1, device_id={'x': x_at(d)}, device_id_type=MESH)
    pl.semaphore_wait(barrier, nc + nx - 1)

    def vec(i):
        return vec_ref[i:i + 1, :]

    def x_cols(d):
        return pl.ds(pl.multiple_of(x_at(d) * width, width), width)

    def scatter_sum(part, dbuf, sbuf, rbuf, base):
        cp = copy(part.at[1 - core], dbuf, base, partner)
        cp.start()
        cp.wait()
        sbuf[...] = (part[core].astype(F32) + dbuf[...].astype(F32)).astype(BF16)
        cps = [copy(sbuf.at[chip_at(d)], rbuf.at[d - 1], base + d, chip_dev(d)) for d in range(1, nc)]
        for cp in cps:
            cp.start()
        total = sbuf[chip].astype(F32)
        for d in range(1, nc):
            cps[d - 1].wait()
            total = total + rbuf[d - 1].astype(F32)
        return total

    def share(buf_at, base):
        far = [copy(buf_at(blk), buf_at(blk), base + d - 1, chip_dev(d)) for d in range(1, nc)]
        for cp in far:
            cp.start()
        near = [copy(buf_at(blk), buf_at(blk), base + nc - 1, partner)]
        near[0].start()
        for d in range(1, nc):
            b = core * nc + chip_at(-d)
            copy(buf_at(b), buf_at(b), base + d - 1, chip_dev(d)).wait_recv()
            cp = copy(buf_at(b), buf_at(b), base + nc - 1 + d, partner)
            cp.start()
            near.append(cp)
        for d in range(nc):
            b = (1 - core) * nc + chip_at(-d)
            copy(buf_at(b), buf_at(b), base + nc - 1 + d, partner).wait_recv()
        for cp in far + near:
            cp.wait_send()

    per = 2 * nc - 1
    base1, base2, base3, base4, base5 = 0, nc, nc + per, 2 * nc + per, 2 * nc + per + nx

    for b in range(nx):
        res = jnp.dot(attn_ref[...], wo_ref[b][...], preferred_element_type=F32).astype(BF16)
        part1[:, :, :, x_cols(b)] = res.reshape(CORES, nc, rows, width)
    total = scatter_sum(part1, dbuf1, sbuf1, rbuf1, base1)
    h_attn = DEEP_ALPHA * hid_ref[...].astype(F32) + total + vec(0)
    z_own = layer_norm(h_attn, vec(1), vec(2))
    zall[blk] = z_own
    share(lambda b: zall.at[b], base2)

    gate = bup_ref[0:1, :].astype(F32)
    val = bup_ref[1:2, :].astype(F32)
    for b in range(nx):
        zb = zall[:, :, x_cols(b)].reshape(ny * rows, width)
        gate = gate + jnp.dot(zb, wup_ref[b][0], preferred_element_type=F32)
        val = val + jnp.dot(zb, wup_ref[b][1], preferred_element_type=F32)
    g = (jax.nn.gelu(gate, approximate=True) * val).astype(BF16)
    for b in range(nx):
        res = jnp.dot(g, wdn_ref[b][...], preferred_element_type=F32).astype(BF16)
        part2[:, :, :, x_cols(b)] = res.reshape(CORES, nc, rows, width)
    total = scatter_sum(part2, dbuf2, sbuf2, rbuf2, base3)
    h_mlp = DEEP_ALPHA * zall[blk].astype(F32) + total + vec(3)
    o = layer_norm(h_mlp, vec(4), vec(5))
    for b in range(nx):
        obuf[b] = o[:, b * width:(b + 1) * width]
    cps = [copy(obuf.at[x_at(d)], out_ref.at[x, blk], base4 + d, {'x': x_at(d)}) for d in range(1, nx)]
    for cp in cps:
        cp.start()
    out_ref[x, blk] = obuf[x]
    for d in range(1, nx):
        copy(obuf.at[x_at(d)], out_ref.at[x_at(-d), blk], base4 + d, {'x': x_at(d)}).wait_recv()
    share(lambda b: out_ref.at[:, b], base5)
    for cp in cps:
        cp.wait_send()


def tail(nx, ny, attn, hid, wo, vecs, wup, bup, wdn):
    nc = ny // CORES
    rows, total_width = hid.shape
    width = total_width // nx
    n_sem = 2 * nc + 2 * (2 * nc - 1) + nx + 1
    vm = pl.BlockSpec(memory_space=pltpu.VMEM)
    reduce_bufs = [pltpu.VMEM((CORES, nc, rows, total_width), BF16), pltpu.VMEM((nc, rows, total_width), BF16),
                   pltpu.VMEM((nc, rows, total_width), BF16), pltpu.VMEM((nc - 1, rows, total_width), BF16)]
    out = pl.pallas_call(
        functools.partial(tail_kernel, nx, ny),
        out_shape=jax.ShapeDtypeStruct((nx, ny, rows, width), BF16),
        in_specs=[vm] * (4 + 3 * nx),
        out_specs=vm,
        scratch_shapes=reduce_bufs + reduce_bufs + [
            pltpu.VMEM((ny, rows, total_width), BF16), pltpu.VMEM((nx, rows, width), BF16),
            pltpu.SemaphoreType.DMA((n_sem,)), pltpu.SemaphoreType.DMA((n_sem,))],
        compiler_params=pltpu.CompilerParams(collective_id=0, has_side_effects=True),
        name='tail',
    )(attn, hid, vecs, bup, *wo, *wup, *wdn)
    return out.reshape(nx * ny * rows, width)


def cache_kernel(n_blocks, k_ref, v_ref, kn_ref, vn_ref, q_ref, lens_ref, lane_ref, ko_ref, vo_ref, attn_ref,
                 qs, sc, acc):
    step = pl.program_id(0)
    slots, heads, dim, _ = k_ref.shape
    own = q_ref.shape[2]
    cols = pl.ds(pl.multiple_of(lax.axis_index('x') * own, own), own)
    total_slots = n_blocks * slots

    @pl.when(step == 0)
    def _():
        qs[...] = q_ref[...].astype(F32)
        acc[...] = jnp.zeros_like(acc)

    def write(src, new, dst, first):
        for s in range(slots):
            hit = lane_ref[...] == (first + s).astype(F32).astype(BF16)
            for h in range(heads):
                for t in range(dim // 16):
                    part = pl.ds(t * 16, 16)
                    dst[s, h, part, :] = jnp.where(hit, new[h, part, :], src[s, h, part, :])

    @pl.when(step < n_blocks)
    def _():
        first = step * slots
        write(k_ref, kn_ref, ko_ref, first)
        for s in range(slots):
            for h in range(heads):
                sc[h, pl.ds(first + s, 1), :] = jnp.sum(
                    ko_ref[s, h, :, cols].astype(F32) * qs[h], axis=0, keepdims=True)

    @pl.when(step == n_blocks - 1)
    def _():
        slot = lax.broadcasted_iota(jnp.int32, (total_slots, own), 0)
        ok = slot <= lens_ref[:, cols]
        for h in range(heads):
            s = jnp.where(ok, sc[h] * (dim ** -0.5), -1e30)
            e = jnp.exp(s - jnp.max(s, axis=0, keepdims=True))
            p = e / jnp.sum(e, axis=0, keepdims=True)
            sc[h] = p.astype(BF16).astype(F32)

    @pl.when(step >= n_blocks)
    def _():
        first = (step - n_blocks) * slots
        write(v_ref, vn_ref, vo_ref, first)
        for h in range(heads):
            a = acc[h]
            for s in range(slots):
                a = a + vo_ref[s, h, :, cols].astype(F32) * sc[h, pl.ds(first + s, 1), :]
            acc[h] = a

    @pl.when(step == 2 * n_blocks - 1)
    def _():
        attn_ref[...] = acc[...].reshape(heads * dim, own).T.astype(BF16)


def cache_step(k_t, v_t, k_new, v_new, q_own, lengths, slots=4):
    total_slots, heads, dim, rows = k_t.shape
    own = q_own.shape[2]
    n = total_slots // slots
    blk = (slots, heads, dim, rows)
    lens = lengths.reshape(1, rows)
    lane = jnp.broadcast_to(lengths.astype(BF16)[None], (16, rows))
    k_spec = pl.BlockSpec(blk, lambda i: (jnp.minimum(i, n - 1), 0, 0, 0))
    v_spec = pl.BlockSpec(blk, lambda i: (jnp.maximum(i - n, 0), 0, 0, 0))
    whole = pl.BlockSpec(memory_space=pltpu.VMEM)
    shape = jax.ShapeDtypeStruct(k_t.shape, k_t.dtype)
    size = 4 * k_t.size * 2
    return pl.pallas_call(
        functools.partial(cache_kernel, n),
        grid=(2 * n,),
        out_shape=(shape, shape, jax.ShapeDtypeStruct((own, heads * dim), BF16)),
        in_specs=[k_spec, v_spec] + [whole] * 5,
        out_specs=(k_spec, v_spec, whole),
        scratch_shapes=[pltpu.VMEM((heads, dim, own), F32), pltpu.VMEM((heads, total_slots, own), F32),
                        pltpu.VMEM((heads, dim, own), F32)],
        cost_estimate=pl.CostEstimate(flops=40 * k_t.size, bytes_accessed=size, transcendentals=0),
        name='cache_step',
    )(k_t, v_t, k_new, v_new, q_own, lens, lane)


def head_kernel(nx, ny, hid_ref, w_ref, b_ref, pos_ref, vec_ref, kn_ref, vn_ref, q_ref, own_ref, vecs_ref,
                hbuf, wbuf, vloc, cos_ref, sin_ref, acc, send, recv):
    nc = ny // CORES
    x, y = lax.axis_index('x'), lax.axis_index('y')
    core, chip = lax.rem(y, CORES), lax.div(y, CORES)
    partner = {'y': chip * CORES + (1 - core)}
    rows, width = hid_ref.shape
    n_out = w_ref.shape[1]
    heads, dim, _ = kn_ref.shape
    half = dim // 2
    piece = rows // ny
    hp, hw = piece // 2, width // 2
    x_right, x_left = {'x': lax.rem(x + 1, nx)}, {'x': lax.rem(x + nx - 1, nx)}

    def y_of(d, same=True):
        return lax.rem(chip + d + nc, nc) * CORES + (core if same else 1 - core)

    c_right, c_left = {'y': y_of(1)}, {'y': y_of(-1)}
    counter = [0]

    def ids(n):
        counter[0] += n
        return list(range(counter[0] - n, counter[0]))

    def copy(src, dst, i, dev):
        return pltpu.make_async_remote_copy(src_ref=src, dst_ref=dst, send_sem=send.at[i], recv_sem=recv.at[i],
                                            device_id=dev, device_id_type=MESH)

    started = []

    def start(src, dst, i, dev):
        cp = copy(src, dst, i, dev)
        cp.start()
        started.append(cp)

    def arrived(ref, i):
        copy(ref, ref, i, partner).wait_recv()

    barrier = pltpu.get_barrier_semaphore()
    peers = [partner, c_right, c_left, x_right, x_left, {'x': lax.rem(x + 2, nx)}]
    for dev in peers:
        pl.semaphore_signal(barrier, inc=1, device_id=dev, device_id_type=MESH)
    pl.semaphore_wait(barrier, len(peers))

    def span(yy, hf):
        return pl.ds(pl.multiple_of(yy * piece + hf * hp, hp), hp)

    def full(yy):
        return pl.ds(pl.multiple_of(yy * piece, piece), piece)

    class Ring:
        def __init__(self, at, right, left):
            self.at, self.right, self.left = at, right, left
            self.ra, self.rb, self.lb, self.la, self.fa, self.fb = ids(6)

        def begin(self):
            at = self.at
            start(at('own', 0, 'src'), at(2, 0, 'dst'), self.ra, self.right)
            start(at('own', 1, 'src'), at(0, 1, 'dst'), self.lb, self.left)
            start(at('own', 1, 'src'), at(2, 1, 'dst'), self.rb, self.right)
            start(at('own', 0, 'src'), at(0, 0, 'dst'), self.la, self.left)

        def forward(self):
            at = self.at
            arrived(at(2, 0, 'here'), self.ra)
            start(at(2, 0, 'here'), at(1, 0, 'fwd_right'), self.fa, self.right)
            arrived(at(0, 1, 'here'), self.lb)
            start(at(0, 1, 'here'), at(1, 1, 'fwd_left'), self.fb, self.left)

        def near(self):
            arrived(self.at(2, 1, 'here'), self.rb)
            arrived(self.at(0, 0, 'here'), self.la)

        def far(self):
            arrived(self.at(1, 0, 'here'), self.fa)
            arrived(self.at(1, 1, 'here'), self.fb)

    def h_at(slot, hf, role):
        if slot == 'own':
            return hid_ref.at[span(y, hf)]
        return hbuf.at[slot, span(y, hf)]

    def w_at(slot, hf, role):
        if slot == 'own':
            return w_ref.at[pl.ds(hf * hw, hw)]
        return wbuf.at[slot, pl.ds(hf * hw, hw)]

    def x_at(j):
        def at(slot, hf, role):
            if slot == 'own' or role == 'dst':
                return hbuf.at[j, span(y, hf)]
            shift = {0: 1, 1: 2, 2: -1}[slot]
            if role == 'fwd_right':
                shift = -1
            elif role == 'fwd_left':
                shift = 1
            return hbuf.at[j, span(y_of(shift), hf)]
        return at

    h_ring = Ring(h_at, x_right, x_left)
    w_ring = Ring(w_at, x_right, x_left)
    x_rings = [Ring(x_at(j), c_right, c_left) for j in range(3)]
    d2d = [ids(nc) for _ in range(3)]
    vec_ids = ids(nx - 1)

    n_vec = vec_ref.shape[0] // width
    for i in range(n_vec):
        vloc[i:i + 1, :] = vec_ref[pl.ds(i * width, width)].reshape(1, width).astype(F32)
    x_cols = pl.ds(pl.multiple_of(x * width, width), width)
    h_ring.begin()
    w_ring.begin()
    for d in range(1, nx):
        start(vloc, vecs_ref.at[:, x_cols], vec_ids[d - 1], {'x': lax.rem(x + d, nx)})

    freq = jnp.exp(lax.broadcasted_iota(jnp.int32, (half, rows), 0).astype(F32) * (-2.0 * math.log(ROPE_BASE) / dim))
    angle = pos_ref[...].astype(F32) * freq
    cos_ref[...] = jnp.cos(angle)
    sin_ref[...] = jnp.sin(angle)

    def product(w, h):
        return lax.dot_general(w.T, h, (((1,), (1,)), ((), ())), preferred_element_type=F32)

    acc[...] = product(w_ref[...], hid_ref[...])
    vecs_ref[:, x_cols] = vloc[...]

    def to_partner(j, d):
        ref = hbuf.at[j, full(y_of(d))]
        start(ref, ref, d2d[j][d % nc], partner)

    h_ring.forward()
    h_ring.near()
    for j in (2, 0):
        x_rings[j].begin()
        to_partner(j, 0)
    w_ring.forward()
    h_ring.far()
    x_rings[1].begin()
    to_partner(1, 0)
    for j in (2, 0, 1):
        x_rings[j].forward()
        x_rings[j].near()
        to_partner(j, 1)
        to_partner(j, -1)
    w_ring.near()
    w_ring.far()
    for j in (2, 0, 1):
        x_rings[j].far()
        to_partner(j, 2)
    for j in (2, 0, 1):
        for d in range(nc):
            arrived(hbuf.at[j, full(y_of(d, False))], d2d[j][d])
        acc[...] += product(wbuf[j], hbuf[j])

    per = own_ref.shape[0]
    first = pl.multiple_of(x * (rows // nx) + (core * nc + chip) * per, per)
    own_ref[:, x_cols] = hid_ref[pl.ds(first, per), :]
    for j in range(3):
        cols = pl.ds(pl.multiple_of(lax.rem(x + j + 1, nx) * width, width), width)
        own_ref[:, cols] = hbuf[j, pl.ds(first, per), :]

    bias = jnp.broadcast_to(b_ref[...].reshape(1, n_out).astype(F32), (128, n_out)).T

    def part(h, which, cols):
        base = (h * 3 + which) * dim
        v = acc[pl.ds(base, dim), cols]
        return (v + bias[base:base + dim, 0:1]).astype(BF16)

    def rotate(v, cols):
        c, s = cos_ref[:, cols], sin_ref[:, cols]
        lo, up = v[:half].astype(F32), v[half:].astype(F32)
        return jnp.concatenate([lo * c - up * s, up * c + lo * s], axis=0).astype(BF16)

    own = q_ref.shape[2]
    own_cols = pl.ds(pl.multiple_of(x * own, own), own)
    for h in range(heads):
        q_ref[h] = rotate(part(h, 0, own_cols), own_cols)
        kn_ref[h] = rotate(part(h, 1, slice(None)), slice(None))
        vn_ref[h] = part(h, 2, slice(None))
    for d in range(1, nx):
        cols = pl.ds(pl.multiple_of(lax.rem(x + nx - d, nx) * width, width), width)
        arrived(vecs_ref.at[:, cols], vec_ids[d - 1])
    for cp in started:
        cp.wait_send()


def head(nx, ny, hidden, w_qkv, b_qkv, positions, vecs, heads, dim):
    rows, width = hidden.shape
    n_out = w_qkv.shape[1]
    n_vec = vecs.shape[0] // width
    vm = pl.BlockSpec(memory_space=pltpu.VMEM)
    n_sem = 6 * 5 + 3 * (ny // CORES) + nx - 1
    shape = jax.ShapeDtypeStruct
    return pl.pallas_call(
        functools.partial(head_kernel, nx, ny),
        out_shape=(shape((heads, dim, rows), BF16), shape((heads, dim, rows), BF16),
                   shape((heads, dim, rows // nx), BF16), shape((rows // (nx * ny), width * nx), BF16),
                   shape((n_vec, width * nx), F32)),
        in_specs=[vm] * 5,
        out_specs=(vm,) * 5,
        scratch_shapes=[pltpu.VMEM((3, rows, width), BF16), pltpu.VMEM((3, width, n_out), BF16),
                        pltpu.VMEM((n_vec, width), F32), pltpu.VMEM((dim // 2, rows), F32),
                        pltpu.VMEM((dim // 2, rows), F32), pltpu.VMEM((n_out, rows), F32),
                        pltpu.SemaphoreType.DMA((n_sem,)), pltpu.SemaphoreType.DMA((n_sem,))],
        compiler_params=pltpu.CompilerParams(collective_id=1, has_side_effects=True),
        name='head',
    )(hidden, w_qkv, b_qkv, positions.reshape(1, rows), vecs)


def solution(mesh):
    nx, ny = mesh.shape['x'], mesh.shape['y']
    cache_spec = P('dp', None, 'y', None)
    width_spec = P('x')
    in_specs = (P('dp', 'x'), P('x', 'y'), P('y'), P('y', 'x'), width_spec, width_spec, width_spec, P('x', None, 'y'), P(None, 'y'), P('y', 'x'), width_spec, width_spec, width_spec, cache_spec, cache_spec, P('dp'), P('dp'))
    out_specs = (P('dp', 'x'), cache_spec, cache_spec)

    def shifted(w, d):
        return lax.ppermute(w, 'x', [((i + d) % nx, i) for i in range(nx)])

    def local_step(hidden, w_qkv, b_qkv, w_out, b_out, attn_gain, attn_shift, w_up, b_up, w_down, b_down, mlp_gain, mlp_shift, k_cache, v_cache, positions, lengths):
        heads, dim = k_cache.shape[2], k_cache.shape[3]
        vecs = jnp.concatenate([b_out, attn_gain, attn_shift, b_down, mlp_gain, mlp_shift, b_out, b_out])
        w_up = jnp.transpose(w_up, (1, 0, 2))
        k_new, v_new, q_own, hid_own, vecs = head(nx, ny, hidden, w_qkv, b_qkv, positions, vecs, heads, dim)
        q_own, w_out, w_up, w_down = lax.optimization_barrier((q_own, w_out, w_up, w_down))
        wo = [w_out] + [shifted(w_out, d) for d in range(1, nx)]
        wup = [w_up] + [shifted(w_up, d) for d in range(1, nx)]
        wdn = [w_down] + [shifted(w_down, d) for d in range(1, nx)]
        k_t, v_t = jnp.transpose(k_cache, (1, 2, 3, 0)), jnp.transpose(v_cache, (1, 2, 3, 0))
        k_t, v_t, attn_own = cache_step(k_t, v_t, k_new, v_new, q_own, lengths)
        k_full, v_full = jnp.transpose(k_t, (3, 0, 1, 2)), jnp.transpose(v_t, (3, 0, 1, 2))
        result = tail(nx, ny, attn_own, hid_own, wo, vecs, wup, b_up, wdn)
        return result, k_full, v_full

    return jax.shard_map(local_step, mesh=mesh, in_specs=in_specs, out_specs=out_specs, check_vma=False)
```

```python
import functools
import math
import jax
import jax.numpy as jnp
from jax import lax
from jax.experimental import pallas as pl
from jax.experimental.pallas import tpu as pltpu
from jax.sharding import PartitionSpec as P

DEEP_ALPHA = math.sqrt(140.0)
LN_EPS = 1e-5
ROPE_BASE = 10000.0
MESH = pl.DeviceIdType.MESH
CORES = 2
N_VEC = 6
F32 = jnp.float32
BF16 = jnp.bfloat16


def layer_norm(h_val, gain, shift):
    mean_row = jnp.mean(h_val, axis=-1, keepdims=True)
    cent = h_val - mean_row
    var_row = jnp.mean(cent * cent, axis=-1, keepdims=True)
    return (cent * lax.rsqrt(var_row + LN_EPS) * gain + shift).astype(BF16)


def tail_kernel(nx, ny, attn_ref, hid_ref, vec_ref, bup_ref, wo_own, wo_all, wup_own, wup_near, wdn_own, out_ref,
                part1, dbuf1, sbuf1, rbuf1, part2, dbuf2, sbuf2, rbuf2, zall, obuf, wup_far, wdn_buf, send, recv):
    nc = ny // CORES
    x, y = lax.axis_index('x'), lax.axis_index('y')
    core, chip = lax.rem(y, CORES), lax.div(y, CORES)
    partner = {'y': chip * CORES + (1 - core)}
    blk = core * nc + chip
    rows = hid_ref.shape[0]
    width = hid_ref.shape[1] // nx

    def chip_at(d):
        return lax.rem(chip + d + nc, nc)

    def x_at(d):
        return lax.rem(x + d + nx, nx)

    def chip_dev(d):
        return {'y': chip_at(d) * CORES + core}

    def copy(src, dst, i, dev):
        return pltpu.make_async_remote_copy(src_ref=src, dst_ref=dst, send_sem=send.at[i], recv_sem=recv.at[i],
                                            device_id=dev, device_id_type=MESH)

    barrier = pltpu.get_barrier_semaphore()
    pl.semaphore_signal(barrier, inc=1, device_id=partner, device_id_type=MESH)
    for d in range(1, nc):
        pl.semaphore_signal(barrier, inc=1, device_id=chip_dev(d), device_id_type=MESH)
    for d in range(1, nx):
        pl.semaphore_signal(barrier, inc=1, device_id={'x': x_at(d)}, device_id_type=MESH)
    pl.semaphore_wait(barrier, nc + nx - 1)

    def vec(i):
        return vec_ref[i:i + 1, :]

    def x_cols(d):
        return pl.ds(pl.multiple_of(x_at(d) * width, width), width)

    hd = wdn_own.shape[0] // 2
    x_right, x_left = {'x': x_at(1)}, {'x': x_at(-1)}
    first = 2 * nc + 2 * (2 * nc - 1) + nx
    lo, hi = pl.ds(0, hd), pl.ds(hd, hd)
    early = [copy(wdn_own.at[lo], wdn_buf.at[2, lo], first, x_right),
             copy(wdn_own.at[hi], wdn_buf.at[0, hi], first + 1, x_left),
             copy(wdn_own.at[hi], wdn_buf.at[2, hi], first + 2, x_right),
             copy(wdn_own.at[lo], wdn_buf.at[0, lo], first + 3, x_left),
             copy(wup_near.at[1, 0], wup_far.at[0], first + 4, x_right),
             copy(wup_near.at[0, 1], wup_far.at[1], first + 5, x_left)]
    for cp in early:
        cp.start()
    wo_ref = [wo_own, wo_all.at[0], wo_all.at[1], wo_all.at[2]]
    wup_ref = [wup_own, wup_near.at[0], wup_far, wup_near.at[1]]
    wdn_ref = [wdn_own, wdn_buf.at[0], wdn_buf.at[1], wdn_buf.at[2]]
    late = [copy(wdn_buf.at[2, lo], wdn_buf.at[1, lo], first + 6, x_right),
            copy(wdn_buf.at[0, hi], wdn_buf.at[1, hi], first + 7, x_left)]

    def pass_on():
        for i in (0, 1):
            early[i].wait_recv()
            late[i].start()

    def scatter_sum(part, dbuf, sbuf, rbuf, base):
        cp = copy(part.at[1 - core], dbuf, base, partner)
        cp.start()
        cp.wait()
        sbuf[...] = (part[core].astype(F32) + dbuf[...].astype(F32)).astype(BF16)
        cps = [copy(sbuf.at[chip_at(d)], rbuf.at[d - 1], base + d, chip_dev(d)) for d in range(1, nc)]
        for cp in cps:
            cp.start()
        total = sbuf[chip].astype(F32)
        for d in range(1, nc):
            cps[d - 1].wait()
            total = total + rbuf[d - 1].astype(F32)
        return total

    def share(buf_at, base, meanwhile=None):
        far = [copy(buf_at(blk), buf_at(blk), base + d - 1, chip_dev(d)) for d in range(1, nc)]
        for cp in far:
            cp.start()
        near = [copy(buf_at(blk), buf_at(blk), base + nc - 1, partner)]
        near[0].start()
        if meanwhile is not None:
            meanwhile()
        for d in range(1, nc):
            b = core * nc + chip_at(-d)
            copy(buf_at(b), buf_at(b), base + d - 1, chip_dev(d)).wait_recv()
            cp = copy(buf_at(b), buf_at(b), base + nc - 1 + d, partner)
            cp.start()
            near.append(cp)
        for d in range(nc):
            b = (1 - core) * nc + chip_at(-d)
            copy(buf_at(b), buf_at(b), base + nc - 1 + d, partner).wait_recv()
        for cp in far + near:
            cp.wait_send()

    per = 2 * nc - 1
    base1, base2, base3, base4, base5 = 0, nc, nc + per, 2 * nc + per, 2 * nc + per + nx

    for b in range(nx):
        res = jnp.dot(attn_ref[...], wo_ref[b][...], preferred_element_type=F32).astype(BF16)
        part1[:, :, :, x_cols(b)] = res.reshape(CORES, nc, rows, width)
    total = scatter_sum(part1, dbuf1, sbuf1, rbuf1, base1)
    h_attn = DEEP_ALPHA * hid_ref[...].astype(F32) + total + vec(0)
    z_own = layer_norm(h_attn, vec(1), vec(2))
    zall[blk] = z_own
    share(lambda b: zall.at[b], base2, pass_on)
    early[4].wait_recv()
    early[5].wait_recv()

    gate = bup_ref[0:1, :].astype(F32)
    val = bup_ref[1:2, :].astype(F32)
    for b in range(nx):
        zb = zall[:, :, x_cols(b)].reshape(ny * rows, width)
        gate = gate + jnp.dot(zb, wup_ref[b][0], preferred_element_type=F32)
        val = val + jnp.dot(zb, wup_ref[b][1], preferred_element_type=F32)
    for cp in early[2:4] + late:
        cp.wait_recv()
    for cp in early + late:
        cp.wait_send()
    g = (jax.nn.gelu(gate, approximate=True) * val).astype(BF16)
    for b in range(nx):
        res = jnp.dot(g, wdn_ref[b][...], preferred_element_type=F32).astype(BF16)
        part2[:, :, :, x_cols(b)] = res.reshape(CORES, nc, rows, width)
    total = scatter_sum(part2, dbuf2, sbuf2, rbuf2, base3)
    h_mlp = DEEP_ALPHA * zall[blk].astype(F32) + total + vec(3)
    o = layer_norm(h_mlp, vec(4), vec(5))
    for b in range(nx):
        obuf[b] = o[:, b * width:(b + 1) * width]
    cps = [copy(obuf.at[x_at(d)], out_ref.at[x, blk], base4 + d, {'x': x_at(d)}) for d in range(1, nx)]
    for cp in cps:
        cp.start()
    out_ref[x, blk] = obuf[x]
    for d in range(1, nx):
        copy(obuf.at[x_at(d)], out_ref.at[x_at(-d), blk], base4 + d, {'x': x_at(d)}).wait_recv()
    share(lambda b: out_ref.at[:, b], base5)
    for cp in cps:
        cp.wait_send()


def tail(nx, ny, attn, hid, vecs, bup, wo, wo_all, wup, wup_near, wdn):
    nc = ny // CORES
    rows, total_width = hid.shape
    width = total_width // nx
    n_sem = 2 * nc + 2 * (2 * nc - 1) + nx + 8
    vm = pl.BlockSpec(memory_space=pltpu.VMEM)
    reduce_bufs = [pltpu.VMEM((CORES, nc, rows, total_width), BF16), pltpu.VMEM((nc, rows, total_width), BF16),
                   pltpu.VMEM((nc, rows, total_width), BF16), pltpu.VMEM((nc - 1, rows, total_width), BF16)]
    out = pl.pallas_call(
        functools.partial(tail_kernel, nx, ny),
        out_shape=jax.ShapeDtypeStruct((nx, ny, rows, width), BF16),
        in_specs=[vm] * 9,
        out_specs=vm,
        scratch_shapes=reduce_bufs + reduce_bufs + [
            pltpu.VMEM((ny, rows, total_width), BF16), pltpu.VMEM((nx, rows, width), BF16),
            pltpu.VMEM(wup.shape, BF16), pltpu.VMEM((3,) + wdn.shape, BF16),
            pltpu.SemaphoreType.DMA((n_sem,)), pltpu.SemaphoreType.DMA((n_sem,))],
        compiler_params=pltpu.CompilerParams(collective_id=0, has_side_effects=True, vmem_limit_bytes=16 * 2**20),
        name='tail',
    )(attn, hid, vecs, bup, wo, wo_all, wup, wup_near, wdn)
    return out.reshape(nx * ny * rows, width)


def update_and_attend(k_ref, v_ref, kn_ref, vn_ref, q_ref, lens_ref, attn_ref, lane, qs, sc, acc, slots, k_here, v_here):
    total_slots, heads, dim, rows = k_ref.shape
    n = total_slots // slots
    own = q_ref.shape[2]
    cols = pl.ds(pl.multiple_of(lax.axis_index('x') * own, own), own)
    lane[...] = jnp.broadcast_to(lens_ref[...].astype(F32), lane.shape).astype(BF16)
    qs[...] = q_ref[...].astype(F32)
    acc[...] = jnp.zeros_like(acc)

    def write(ref, new, first):
        for s in range(slots):
            hit = lane[...] == (first + s).astype(F32).astype(BF16)
            for h in range(heads):
                for t in range(dim // 16):
                    part = pl.ds(t * 16, 16)
                    ref[first + s, h, part, :] = jnp.where(hit, new[h, part, :], ref[first + s, h, part, :])

    def k_step(i, carry):
        first = i * slots
        write(k_ref, kn_ref, first)
        for s in range(slots):
            for h in range(heads):
                sc[h, pl.ds(first + s, 1), :] = jnp.sum(
                    k_ref[first + s, h, :, cols].astype(F32) * qs[h], axis=0, keepdims=True)
        return carry

    k_here()
    lax.fori_loop(0, n, k_step, 0)
    slot_id = lax.broadcasted_iota(jnp.int32, (total_slots, own), 0)
    ok = slot_id <= lens_ref[:, cols]
    for h in range(heads):
        s = jnp.where(ok, sc[h] * (dim ** -0.5), -1e30)
        e = jnp.exp(s - jnp.max(s, axis=0, keepdims=True))
        p = e / jnp.sum(e, axis=0, keepdims=True)
        sc[h] = p.astype(BF16).astype(F32)

    def v_step(i, carry):
        first = i * slots
        write(v_ref, vn_ref, first)
        for h in range(heads):
            a = acc[h]
            for s in range(slots):
                a = a + v_ref[first + s, h, :, cols].astype(F32) * sc[h, pl.ds(first + s, 1), :]
            acc[h] = a
        return carry

    v_here()
    lax.fori_loop(0, n, v_step, 0)
    attn_ref[...] = acc[...].reshape(heads * dim, own).T.astype(BF16)


def head_kernel(nx, ny, hid_ref, w_ref, b_ref, pos_ref, lens_ref, wo_ref, wup_ref, k_ref, v_ref, *refs):
    vec_refs, (attn_ref, own_ref, vecs_ref, wo_all, wup_near, kc_ref, vc_ref, kn_ref, vn_ref, q_ref,
               lane, qs, sc, att,
               hbuf, wbuf, vloc, cos_ref, sin_ref, acc, send, recv, load) = refs[:N_VEC], refs[N_VEC:]
    nc = ny // CORES
    x, y = lax.axis_index('x'), lax.axis_index('y')
    core, chip = lax.rem(y, CORES), lax.div(y, CORES)
    partner = {'y': chip * CORES + (1 - core)}
    rows, width = hid_ref.shape
    n_out = w_ref.shape[1]
    heads, dim, _ = kn_ref.shape
    half = dim // 2
    piece = rows // ny
    hp, hw = piece // 2, width // 2
    x_right, x_left = {'x': lax.rem(x + 1, nx)}, {'x': lax.rem(x + nx - 1, nx)}

    def y_of(d, same=True):
        return lax.rem(chip + d + nc, nc) * CORES + (core if same else 1 - core)

    c_right, c_left = {'y': y_of(1)}, {'y': y_of(-1)}
    counter = [0]

    def ids(n):
        counter[0] += n
        return list(range(counter[0] - n, counter[0]))

    def copy(src, dst, i, dev):
        return pltpu.make_async_remote_copy(src_ref=src, dst_ref=dst, send_sem=send.at[i], recv_sem=recv.at[i],
                                            device_id=dev, device_id_type=MESH)

    started = []

    def start(src, dst, i, dev):
        cp = copy(src, dst, i, dev)
        cp.start()
        started.append(cp)

    def arrived(ref, i):
        copy(ref, ref, i, partner).wait_recv()

    barrier = pltpu.get_barrier_semaphore()
    peers = [partner, c_right, c_left, x_right, x_left, {'x': lax.rem(x + 2, nx)}]
    n_load = load.shape[1]
    step = k_ref.shape[0] // n_load
    loads = [pltpu.make_async_copy(src.at[pl.ds(i * step, step)], dst.at[pl.ds(i * step, step)], load.at[j, i])
             for j, (src, dst) in enumerate(((k_ref, kc_ref), (v_ref, vc_ref))) for i in range(n_load)]
    for cp in loads:
        cp.start()
    for dev in peers:
        pl.semaphore_signal(barrier, inc=1, device_id=dev, device_id_type=MESH)
    pl.semaphore_wait(barrier, len(peers))

    def span(yy, hf):
        return pl.ds(pl.multiple_of(yy * piece + hf * hp, hp), hp)

    def full(yy):
        return pl.ds(pl.multiple_of(yy * piece, piece), piece)

    class Ring:
        def __init__(self, at, right, left):
            self.at, self.right, self.left = at, right, left
            self.ra, self.rb, self.lb, self.la, self.fa, self.fb = ids(6)

        def begin(self):
            at = self.at
            start(at('own', 0, 'src'), at(2, 0, 'dst'), self.ra, self.right)
            start(at('own', 1, 'src'), at(0, 1, 'dst'), self.lb, self.left)
            start(at('own', 1, 'src'), at(2, 1, 'dst'), self.rb, self.right)
            start(at('own', 0, 'src'), at(0, 0, 'dst'), self.la, self.left)

        def forward(self):
            at = self.at
            arrived(at(2, 0, 'here'), self.ra)
            start(at(2, 0, 'here'), at(1, 0, 'fwd_right'), self.fa, self.right)
            arrived(at(0, 1, 'here'), self.lb)
            start(at(0, 1, 'here'), at(1, 1, 'fwd_left'), self.fb, self.left)

        def near(self):
            arrived(self.at(2, 1, 'here'), self.rb)
            arrived(self.at(0, 0, 'here'), self.la)

        def far(self):
            arrived(self.at(1, 0, 'here'), self.fa)
            arrived(self.at(1, 1, 'here'), self.fb)

    def h_at(slot, hf, role):
        if slot == 'own':
            return hid_ref.at[span(y, hf)]
        return hbuf.at[slot, span(y, hf)]

    def w_at(slot, hf, role):
        if slot == 'own':
            return w_ref.at[pl.ds(hf * hw, hw)]
        return wbuf.at[slot, pl.ds(hf * hw, hw)]

    def x_at(j):
        def at(slot, hf, role):
            if slot == 'own' or role == 'dst':
                return hbuf.at[j, span(y, hf)]
            shift = {0: 1, 1: 2, 2: -1}[slot]
            if role == 'fwd_right':
                shift = -1
            elif role == 'fwd_left':
                shift = 1
            return hbuf.at[j, span(y_of(shift), hf)]
        return at

    ho = wo_ref.shape[0] // 2

    def o_at(slot, hf, role):
        if slot == 'own':
            return wo_ref.at[pl.ds(hf * ho, ho)]
        return wo_all.at[slot, pl.ds(hf * ho, ho)]

    h_ring = Ring(h_at, x_right, x_left)
    w_ring = Ring(w_at, x_right, x_left)
    o_ring = Ring(o_at, x_right, x_left)
    up_ids = ids(2)
    x_rings = [Ring(x_at(j), c_right, c_left) for j in range(3)]
    d2d = [ids(nc) for _ in range(3)]
    vec_ids = ids(nx - 1)

    for i in range(N_VEC):
        vloc[i:i + 1, :] = vec_refs[i][...].reshape(1, width).astype(F32)
    x_cols = pl.ds(pl.multiple_of(x * width, width), width)
    h_ring.begin()
    w_ring.begin()
    for d in range(1, nx):
        start(vloc, vecs_ref.at[:, x_cols], vec_ids[d - 1], {'x': lax.rem(x + d, nx)})

    freq = jnp.exp(lax.broadcasted_iota(jnp.int32, (half, rows), 0).astype(F32) * (-2.0 * math.log(ROPE_BASE) / dim))
    angle = pos_ref[...].astype(F32) * freq
    cos_ref[...] = jnp.cos(angle)
    sin_ref[...] = jnp.sin(angle)

    def product(w, h):
        return lax.dot_general(w.T, h, (((1,), (1,)), ((), ())), preferred_element_type=F32)

    acc[...] = product(w_ref[...], hid_ref[...])
    vecs_ref[:, x_cols] = vloc[...]

    def to_partner(j, d):
        ref = hbuf.at[j, full(y_of(d))]
        start(ref, ref, d2d[j][d % nc], partner)

    h_ring.forward()
    h_ring.near()
    for j in (2, 0):
        x_rings[j].begin()
        to_partner(j, 0)
    w_ring.forward()
    h_ring.far()
    x_rings[1].begin()
    to_partner(1, 0)
    for j in (2, 0, 1):
        x_rings[j].forward()
        x_rings[j].near()
        to_partner(j, 1)
        to_partner(j, -1)
        if j == 2:
            w_ring.near()
            o_ring.begin()
            start(wup_ref, wup_near.at[1], up_ids[0], x_right)
            start(wup_ref, wup_near.at[0], up_ids[1], x_left)
    w_ring.far()
    o_ring.forward()
    for j in (2, 0, 1):
        x_rings[j].far()
        to_partner(j, 2)
    for j in (2, 0, 1):
        for d in range(nc):
            arrived(hbuf.at[j, full(y_of(d, False))], d2d[j][d])
        acc[...] += product(wbuf[j], hbuf[j])

    per = own_ref.shape[0]
    first = pl.multiple_of(x * (rows // nx) + (core * nc + chip) * per, per)
    own_ref[:, x_cols] = hid_ref[pl.ds(first, per), :]
    for j in range(3):
        cols = pl.ds(pl.multiple_of(lax.rem(x + j + 1, nx) * width, width), width)
        own_ref[:, cols] = hbuf[j, pl.ds(first, per), :]

    bias = jnp.broadcast_to(b_ref[...].reshape(1, n_out).astype(F32), (128, n_out)).T

    def part(h, which, cols):
        base = (h * 3 + which) * dim
        v = acc[pl.ds(base, dim), cols]
        return (v + bias[base:base + dim, 0:1]).astype(BF16)

    def rotate(v, cols):
        c, s = cos_ref[:, cols], sin_ref[:, cols]
        lo, up = v[:half].astype(F32), v[half:].astype(F32)
        return jnp.concatenate([lo * c - up * s, up * c + lo * s], axis=0).astype(BF16)

    own = q_ref.shape[2]
    own_cols = pl.ds(pl.multiple_of(x * own, own), own)
    for h in range(heads):
        q_ref[h] = rotate(part(h, 0, own_cols), own_cols)
        kn_ref[h] = rotate(part(h, 1, slice(None)), slice(None))
        vn_ref[h] = part(h, 2, slice(None))
    for d in range(1, nx):
        cols = pl.ds(pl.multiple_of(lax.rem(x + nx - d, nx) * width, width), width)
        arrived(vecs_ref.at[:, cols], vec_ids[d - 1])
    o_ring.near()

    def k_here():
        for cp in loads[:n_load]:
            cp.wait()

    def v_here():
        for cp in loads[n_load:]:
            cp.wait()

    update_and_attend(kc_ref, vc_ref, kn_ref, vn_ref, q_ref, lens_ref, attn_ref, lane, qs, sc, att, 4, k_here, v_here)
    o_ring.far()
    arrived(wup_near.at[1], up_ids[0])
    arrived(wup_near.at[0], up_ids[1])
    for cp in started:
        cp.wait_send()


def head(nx, ny, hidden, w_qkv, b_qkv, positions, lengths, w_out, w_up, k_t, v_t, vecs):
    rows, width = hidden.shape
    n_out = w_qkv.shape[1]
    _, heads, dim, _ = k_t.shape
    n_vec = 8
    own = rows // nx
    vm = pl.BlockSpec(memory_space=pltpu.VMEM)
    hbm = pl.BlockSpec(memory_space=pl.ANY)
    n_sem = 6 * 6 + 2 + 3 * (ny // CORES) + nx - 1
    shape = pltpu.VMEM
    return pl.pallas_call(
        functools.partial(head_kernel, nx, ny),
        out_shape=(shape((rows // nx, heads * dim), BF16), shape((rows // (nx * ny), width * nx), BF16),
                   shape((n_vec, width * nx), F32), shape((3,) + w_out.shape, BF16), shape((2,) + w_up.shape, BF16),
                   shape(k_t.shape, BF16), shape(v_t.shape, BF16)),
        in_specs=[vm] * 6 + [hbm] * 3 + [vm] * N_VEC,
        out_specs=(vm,) * 7,
        scratch_shapes=[pltpu.VMEM((heads, dim, rows), BF16), pltpu.VMEM((heads, dim, rows), BF16),
                        pltpu.VMEM((heads, dim, own), BF16), pltpu.VMEM((16, rows), BF16),
                        pltpu.VMEM((heads, dim, own), F32), pltpu.VMEM((heads, k_t.shape[0], own), F32),
                        pltpu.VMEM((heads, dim, own), F32), pltpu.VMEM((3, rows, width), BF16), pltpu.VMEM((3, width, n_out), BF16),
                        pltpu.VMEM((n_vec, width), F32), pltpu.VMEM((dim // 2, rows), F32),
                        pltpu.VMEM((dim // 2, rows), F32), pltpu.VMEM((n_out, rows), F32),
                        pltpu.SemaphoreType.DMA((n_sem,)), pltpu.SemaphoreType.DMA((n_sem,)),
                        pltpu.SemaphoreType.DMA((2, 8))],
        compiler_params=pltpu.CompilerParams(collective_id=1, has_side_effects=True, vmem_limit_bytes=16 * 2**20),
        name='head',
    )(hidden, w_qkv, b_qkv, positions.reshape(1, rows), lengths.reshape(1, rows), w_out, w_up, k_t, v_t, *vecs)


def solution(mesh):
    nx, ny = mesh.shape['x'], mesh.shape['y']
    cache_spec = P('dp', None, 'y', None)
    width_spec = P('x')
    in_specs = (P('dp', 'x'), P('x', 'y'), P('y'), P('y', 'x'), width_spec, width_spec, width_spec, P('x', None, 'y'), P(None, 'y'), P('y', 'x'), width_spec, width_spec, width_spec, cache_spec, cache_spec, P('dp'), P('dp'))
    out_specs = (P('dp', 'x'), cache_spec, cache_spec)

    def local_step(hidden, w_qkv, b_qkv, w_out, b_out, attn_gain, attn_shift, w_up, b_up, w_down, b_down, mlp_gain, mlp_shift, k_cache, v_cache, positions, lengths):
        k_t, v_t = jnp.transpose(k_cache, (1, 2, 3, 0)), jnp.transpose(v_cache, (1, 2, 3, 0))
        w_up = jnp.transpose(w_up, (1, 0, 2))
        vecs = (b_out, attn_gain, attn_shift, b_down, mlp_gain, mlp_shift)
        attn_own, hid_own, vecs, wo_all, wup_near, k_t, v_t = head(
            nx, ny, hidden, w_qkv, b_qkv, positions, lengths, w_out, w_up, k_t, v_t, vecs)
        result = tail(nx, ny, attn_own, hid_own, vecs, b_up, w_out, wo_all, w_up, wup_near, w_down)
        k_full, v_full = jnp.transpose(k_t, (3, 0, 1, 2)), jnp.transpose(v_t, (3, 0, 1, 2))
        return result, k_full, v_full

    return jax.shard_map(local_step, mesh=mesh, in_specs=in_specs, out_specs=out_specs, check_vma=False)
```

```python
import functools
import math
import jax
import jax.numpy as jnp
from jax import lax
from jax.experimental import pallas as pl
from jax.experimental.pallas import tpu as pltpu
from jax.sharding import PartitionSpec as P

DEEP_ALPHA = math.sqrt(140.0)
LN_EPS = 1e-5
ROPE_BASE = 10000.0
MESH = pl.DeviceIdType.MESH
CORES = 2
N_VEC = 6
N_LOAD = 1
GROUP = 4
F32 = jnp.float32
BF16 = jnp.bfloat16


def layer_norm(h_val, gain, shift):
    mean_row = jnp.mean(h_val, axis=-1, keepdims=True)
    cent = h_val - mean_row
    var_row = jnp.mean(cent * cent, axis=-1, keepdims=True)
    return (cent * lax.rsqrt(var_row + LN_EPS) * gain + shift).astype(BF16)


def layer_kernel(nx, ny, hid_in, wqkv_in, wo_in, wup_in, wdn_in, bup_in, bqkv_in, pos_in, lens_in, k_in, v_in, *refs):
    vec_in, refs = refs[:N_VEC], refs[N_VEC:]
    out_ref, kc, vc = refs[:3]
    vec_own, refs = refs[3:3 + N_VEC], refs[3 + N_VEC:]
    (hid, wqkv, wo_own, wup_own, wdn_own, bup, bqkv, pos, lens, qpart, qrecv, qown, kvn, qs, sc, lane,
     wo_far, wup_far, wdn_far, vloc, vecs, hid_own, part1, dbuf1, sbuf1, rbuf1, part2, dbuf2, sbuf2, rbuf2,
     zall, obuf, send, recv, load, cache_load) = refs
    nc = ny // CORES
    x, y = lax.axis_index('x'), lax.axis_index('y')
    core, chip = lax.rem(y, CORES), lax.div(y, CORES)
    partner = {'y': chip * CORES + (1 - core)}
    blk = core * nc + chip
    total_slots, heads, dim, all_rows = k_in.shape
    half = dim // 2
    width = hid_in.shape[1]
    own = all_rows // nx
    per = own // ny
    n_out = wqkv_in.shape[1]

    def chip_at(d):
        return lax.rem(chip + d + nc, nc)

    def x_at(d):
        return lax.rem(x + d + nx, nx)

    def chip_dev(d):
        return {'y': chip_at(d) * CORES + core}

    def x_dev(d):
        return {'x': x_at(d)}

    def x_cols(d):
        return pl.ds(pl.multiple_of(x_at(d) * width, width), width)

    def x_rows(d):
        return pl.ds(pl.multiple_of(x_at(d) * own, own), own)

    cols = x_rows(0)
    counter = [0]
    started = []

    def ids(n):
        counter[0] += n
        return list(range(counter[0] - n, counter[0]))

    def copy(src, dst, i, dev):
        return pltpu.make_async_remote_copy(src_ref=src, dst_ref=dst, send_sem=send.at[i], recv_sem=recv.at[i],
                                            device_id=dev, device_id_type=MESH)

    def start(src, dst, i, dev):
        cp = copy(src, dst, i, dev)
        cp.start()
        started.append(cp)

    def arrived(ref, i):
        copy(ref, ref, i, partner).wait_recv()

    pairs = [(hid_in, hid), (wqkv_in, wqkv), (bqkv_in, bqkv), (pos_in, pos), (lens_in, lens), (bup_in, bup),
             (wo_in, wo_own), (wup_in, wup_own), (wdn_in, wdn_own)] + list(zip(vec_in, vec_own))
    loads = [pltpu.make_async_copy(src, dst, load.at[i]) for i, (src, dst) in enumerate(pairs)]
    for cp in loads:
        cp.start()
    step = total_slots // N_LOAD
    cache_loads = [[pltpu.make_async_copy(src.at[pl.ds(i * step, step)], dst.at[pl.ds(i * step, step)],
                                          cache_load.at[j, i]) for i in range(N_LOAD)]
                   for j, (src, dst) in enumerate(((k_in, kc), (v_in, vc)))]

    barrier = pltpu.get_barrier_semaphore()
    peers = [partner] + [chip_dev(d) for d in range(1, nc)] + [x_dev(d) for d in range(1, nx)]
    for dev in peers:
        pl.semaphore_signal(barrier, inc=1, device_id=dev, device_id_type=MESH)
    for cp in loads:
        cp.wait()
    w_t = wqkv[...].T

    def product(d):
        return lax.dot_general(w_t, hid[x_rows(d), :], (((1,), (1,)), ((), ())), preferred_element_type=F32)

    order = [2, 1, 3]
    for d in order:
        qpart[d - 1] = product(d).astype(BF16)
    pl.semaphore_wait(barrier, len(peers))

    q_ids, wo_ids, hid_ids, vec_ids, kv_ids = (ids(nx - 1) for _ in range(5))
    for d in order:
        start(qpart.at[d - 1], qrecv.at[d - 1], q_ids[d - 1], x_dev(d))
    for i in range(N_VEC):
        vloc[i:i + 1, :] = vec_own[i][...].reshape(1, width).astype(F32)

    def my_rows(d):
        return pl.ds(pl.multiple_of(x_at(d) * own + blk * per, per), per)

    for d in order:
        start(wo_own, wo_far.at[d - 1], wo_ids[d - 1], x_dev(d))
        start(hid.at[my_rows(d)], hid_own.at[:, x_cols(0)], hid_ids[d - 1], x_dev(d))
        start(vloc, vecs.at[:, x_cols(0)], vec_ids[d - 1], x_dev(d))

    class Ring:
        def __init__(self, piece, buf):
            self.piece, self.buf = piece, buf
            self.ra, self.rb, self.lb, self.la, self.fa, self.fb = ids(6)

        def begin(self):
            start(self.piece(0), self.buf(2, 0), self.ra, x_dev(1))
            start(self.piece(1), self.buf(0, 1), self.lb, x_dev(-1))
            start(self.piece(1), self.buf(2, 1), self.rb, x_dev(1))
            start(self.piece(0), self.buf(0, 0), self.la, x_dev(-1))

        def forward(self):
            arrived(self.buf(2, 0), self.ra)
            start(self.buf(2, 0), self.buf(1, 0), self.fa, x_dev(1))
            arrived(self.buf(0, 1), self.lb)
            start(self.buf(0, 1), self.buf(1, 1), self.fb, x_dev(-1))

        def near(self):
            arrived(self.buf(2, 1), self.rb)
            arrived(self.buf(0, 0), self.la)

        def far(self):
            arrived(self.buf(1, 0), self.fa)
            arrived(self.buf(1, 1), self.fb)

    hd = wdn_own.shape[0] // 2
    up_ring = Ring(lambda h: wup_own.at[h], lambda s, h: wup_far.at[s, h])
    down_ring = Ring(lambda h: wdn_own.at[pl.ds(h * hd, hd)], lambda s, h: wdn_far.at[s, pl.ds(h * hd, hd)])
    up_ring.begin()
    down_ring.begin()
    for group in cache_loads:
        for cp in group:
            cp.start()

    qown[...] = product(0)
    vecs[:, x_cols(0)] = vloc[...]
    hid_own[:, x_cols(0)] = hid[my_rows(0), :]
    freq = jnp.exp(lax.broadcasted_iota(jnp.int32, (half, own), 0).astype(F32) * (-2.0 * math.log(ROPE_BASE) / dim))
    angle = pos[:, cols].astype(F32) * freq
    cos_t, sin_t = jnp.cos(angle), jnp.sin(angle)
    bias = jnp.broadcast_to(bqkv[...].reshape(1, n_out).astype(F32), (128, n_out)).T
    lane[...] = jnp.broadcast_to(lens[...].astype(F32), lane.shape).astype(BF16)

    total = qown[...]
    for d in order:
        arrived(qrecv.at[d - 1], q_ids[d - 1])
        total = total + qrecv[d - 1].astype(F32)
    qkv = (total + bias[:, 0:1]).astype(BF16)

    def rotate(v):
        lo, up = v[:half].astype(F32), v[half:].astype(F32)
        return jnp.concatenate([lo * cos_t - up * sin_t, up * cos_t + lo * sin_t], axis=0).astype(BF16)

    for h in range(heads):
        base = 3 * h * dim
        qs[h] = rotate(qkv[base:base + dim]).astype(F32)
        kvn[0, h, :, cols] = rotate(qkv[base + dim:base + 2 * dim])
        kvn[1, h, :, cols] = qkv[base + 2 * dim:base + 3 * dim]

    def score_step(i, carry):
        for s in range(GROUP):
            for h in range(heads):
                sc[h, pl.ds(i * GROUP + s, 1), :] = jnp.sum(
                    kc[i * GROUP + s, h, :, cols].astype(F32) * qs[h], axis=0, keepdims=True)
        return carry

    for cp in cache_loads[0]:
        cp.wait()
    lax.fori_loop(0, total_slots // GROUP, score_step, 0)
    slot_id = lax.broadcasted_iota(jnp.int32, (total_slots, own), 0)
    own_len = lens[:, cols]
    ok, hit = slot_id <= own_len, slot_id == own_len
    p_new = []
    for h in range(heads):
        s_new = jnp.sum(kvn[0, h, :, cols].astype(F32) * qs[h], axis=0, keepdims=True)
        s = jnp.where(hit, s_new, sc[h]) * (dim ** -0.5)
        s = jnp.where(ok, s, -1e30)
        e = jnp.exp(s - jnp.max(s, axis=0, keepdims=True))
        p = (e / jnp.sum(e, axis=0, keepdims=True)).astype(BF16).astype(F32)
        p_new.append(jnp.sum(jnp.where(hit, p, 0.0), axis=0, keepdims=True))
        sc[h] = jnp.where(hit, 0.0, p)
    for h in range(heads):
        qs[h] = p_new[h] * kvn[1, h, :, cols].astype(F32)

    def mix_step(i, carry):
        for h in range(heads):
            a = qs[h]
            for s in range(GROUP):
                a = a + vc[i * GROUP + s, h, :, cols].astype(F32) * sc[h, pl.ds(i * GROUP + s, 1), :]
            qs[h] = a
        return carry

    for cp in cache_loads[1]:
        cp.wait()
    lax.fori_loop(0, total_slots // GROUP, mix_step, 0)
    attn = qs[...].reshape(heads * dim, own).T.astype(BF16)

    def update(ref, which):
        def write(i, carry):
            for s in range(GROUP):
                slot_hit = lane[...] == (i * GROUP + s).astype(F32).astype(BF16)
                for h in range(heads):
                    for t in range(dim // 16):
                        part = pl.ds(t * 16, 16)
                        ref[i * GROUP + s, h, part, :] = jnp.where(
                            slot_hit, kvn[which, h, part, :], ref[i * GROUP + s, h, part, :])
            return carry

        lax.fori_loop(0, total_slots // GROUP, write, 0)

    def vec(i):
        return vecs[i:i + 1, :]

    def scatter_sum(part, dbuf, sbuf, rbuf):
        base = ids(nc)
        start(part.at[1 - core], dbuf, base[0], partner)
        arrived(dbuf, base[0])
        sbuf[...] = (part[core].astype(F32) + dbuf[...].astype(F32)).astype(BF16)
        for d in (2, 1, 3):
            start(sbuf.at[chip_at(d)], rbuf.at[d - 1], base[d], chip_dev(d))
        sums = sbuf[chip].astype(F32)
        for d in range(1, nc):
            arrived(rbuf.at[d - 1], base[d])
            sums = sums + rbuf[d - 1].astype(F32)
        return sums

    def share(buf_at, meanwhile):
        far, near = ids(nc), ids(nc)
        for d in (2, 1, 3):
            start(buf_at(blk), buf_at(blk), far[d], chip_dev(d))
        start(buf_at(blk), buf_at(blk), near[0], partner)
        meanwhile()
        for d in (1, 3, 2):
            ref = buf_at(core * nc + chip_at(-d))
            arrived(ref, far[d])
            start(ref, ref, near[d], partner)
        for d in (0, 1, 3, 2):
            arrived(buf_at((1 - core) * nc + chip_at(-d)), near[d])

    def put(part, d, value):
        part[:, :, :, x_cols(d)] = value.astype(BF16).reshape(CORES, nc, per, width)

    put(part1, 0, jnp.dot(attn, wo_own[...], preferred_element_type=F32))
    for d in order:
        arrived(wo_far.at[d - 1], wo_ids[d - 1])
        put(part1, -d, jnp.dot(attn, wo_far[d - 1], preferred_element_type=F32))
    total = scatter_sum(part1, dbuf1, sbuf1, rbuf1)
    for d in range(1, nx):
        arrived(hid_own.at[:, x_cols(-d)], hid_ids[d - 1])
        arrived(vecs.at[:, x_cols(-d)], vec_ids[d - 1])
    h_attn = DEEP_ALPHA * hid_own[...].astype(F32) + total + vec(0)
    zall[blk] = layer_norm(h_attn, vec(1), vec(2))
    share(lambda b: zall.at[b], up_ring.forward)
    down_ring.forward()
    for d in order:
        mine = kvn.at[:, :, :, cols]
        start(mine, mine, kv_ids[d - 1], x_dev(d))

    ups = [(0, wup_own), (1, wup_far.at[0]), (-1, wup_far.at[2]), (2, wup_far.at[1])]
    downs = [(0, wdn_own), (1, wdn_far.at[0]), (-1, wdn_far.at[2]), (2, wdn_far.at[1])]
    gate = bup[0:1, :].astype(F32)
    val = bup[1:2, :].astype(F32)
    up_ring.near()
    for d, w in ups:
        if d == 2:
            up_ring.far()
        zb = zall[:, :, x_cols(d)].reshape(own, width)
        gate = gate + jnp.dot(zb, w[0], preferred_element_type=F32)
        val = val + jnp.dot(zb, w[1], preferred_element_type=F32)
    g = (jax.nn.gelu(gate, approximate=True) * val).astype(BF16)
    down_ring.near()
    for d, w in downs:
        if d == 2:
            down_ring.far()
        put(part2, d, jnp.dot(g, w[...], preferred_element_type=F32))
    total = scatter_sum(part2, dbuf2, sbuf2, rbuf2)
    h_mlp = DEEP_ALPHA * zall[blk].astype(F32) + total + vec(3)
    o = layer_norm(h_mlp, vec(4), vec(5))
    for b in range(nx):
        obuf[b] = o[:, b * width:(b + 1) * width]
    out_ids = ids(nx)
    for d in order:
        start(obuf.at[x_at(d)], out_ref.at[x, blk], out_ids[d], x_dev(d))
    out_ref[x, blk] = obuf[x]
    for d in range(1, nx):
        arrived(kvn.at[:, :, :, x_rows(-d)], kv_ids[d - 1])
    update(kc, 0)
    for d in range(1, nx):
        arrived(out_ref.at[x_at(-d), blk], out_ids[d])
    share(lambda b: out_ref.at[:, b], lambda: update(vc, 1))
    for cp in started:
        cp.wait_send()


def layer(nx, ny, hidden, w_qkv, w_out, w_up, w_down, b_up, b_qkv, positions, lengths, k_t, v_t, vecs):
    nc = ny // CORES
    rows, width = hidden.shape
    total_slots, heads, dim, _ = k_t.shape
    own = rows // nx
    per = own // ny
    total_width = width * nx
    n_out = w_qkv.shape[1]
    n_sem = 5 * (nx - 1) + 12 + 6 * nc + nx
    hbm = pl.BlockSpec(memory_space=pltpu.HBM)
    vm = pl.BlockSpec(memory_space=pltpu.VMEM)
    reduce_bufs = [pltpu.VMEM((CORES, nc, per, total_width), BF16), pltpu.VMEM((nc, per, total_width), BF16),
                   pltpu.VMEM((nc, per, total_width), BF16), pltpu.VMEM((nc - 1, per, total_width), BF16)]
    ins = (hidden, w_qkv, w_out, w_up, w_down, b_up, b_qkv, positions.reshape(1, rows), lengths.reshape(1, rows))
    out, k_t, v_t = pl.pallas_call(
        functools.partial(layer_kernel, nx, ny),
        out_shape=(jax.ShapeDtypeStruct((nx, ny, per, width), BF16), pltpu.VMEM(k_t.shape, BF16),
                   pltpu.VMEM(v_t.shape, BF16)),
        in_specs=[hbm] * (len(ins) + 2 + N_VEC),
        out_specs=(vm,) * 3,
        scratch_shapes=[pltpu.VMEM(v.shape, BF16) for v in vecs] + [
            pltpu.VMEM(a.shape, a.dtype) for a in (hidden, w_qkv, w_out, w_up, w_down, b_up, b_qkv, ins[7], ins[8])] + [
            pltpu.VMEM((nx - 1, n_out, own), BF16), pltpu.VMEM((nx - 1, n_out, own), BF16),
            pltpu.VMEM((n_out, own), F32), pltpu.VMEM((2, heads, dim, rows), BF16),
            pltpu.VMEM((heads, dim, own), F32), pltpu.VMEM((heads, total_slots, own), F32),
            pltpu.VMEM((16, rows), BF16), pltpu.VMEM((nx - 1,) + w_out.shape, BF16),
            pltpu.VMEM((nx - 1,) + w_up.shape, BF16), pltpu.VMEM((nx - 1,) + w_down.shape, BF16),
            pltpu.VMEM((8, width), F32), pltpu.VMEM((8, total_width), F32), pltpu.VMEM((per, total_width), BF16),
        ] + reduce_bufs + reduce_bufs + [
            pltpu.VMEM((ny, per, total_width), BF16), pltpu.VMEM((nx, per, width), BF16),
            pltpu.SemaphoreType.DMA((n_sem,)), pltpu.SemaphoreType.DMA((n_sem,)),
            pltpu.SemaphoreType.DMA((len(ins) + N_VEC,)), pltpu.SemaphoreType.DMA((2, N_LOAD))],
        compiler_params=pltpu.CompilerParams(collective_id=0, has_side_effects=True, vmem_limit_bytes=24 * 2**20),
        name='layer',
    )(*ins, k_t, v_t, *vecs)
    return out.reshape(rows, width), k_t, v_t


def solution(mesh):
    nx, ny = mesh.shape['x'], mesh.shape['y']
    cache_spec = P('dp', None, 'y', None)
    width_spec = P('x')
    in_specs = (P('dp', 'x'), P('x', 'y'), P('y'), P('y', 'x'), width_spec, width_spec, width_spec, P('x', None, 'y'), P(None, 'y'), P('y', 'x'), width_spec, width_spec, width_spec, cache_spec, cache_spec, P('dp'), P('dp'))
    out_specs = (P('dp', 'x'), cache_spec, cache_spec)

    def local_step(hidden, w_qkv, b_qkv, w_out, b_out, attn_gain, attn_shift, w_up, b_up, w_down, b_down, mlp_gain, mlp_shift, k_cache, v_cache, positions, lengths):
        k_t, v_t = jnp.transpose(k_cache, (1, 2, 3, 0)), jnp.transpose(v_cache, (1, 2, 3, 0))
        w_up = jnp.transpose(w_up, (1, 0, 2))
        vecs = (b_out, attn_gain, attn_shift, b_down, mlp_gain, mlp_shift)
        result, k_t, v_t = layer(nx, ny, hidden, w_qkv, w_out, w_up, w_down, b_up, b_qkv, positions, lengths, k_t, v_t, vecs)
        k_full, v_full = jnp.transpose(k_t, (3, 0, 1, 2)), jnp.transpose(v_t, (3, 0, 1, 2))
        return result, k_full, v_full

    return jax.shard_map(local_step, mesh=mesh, in_specs=in_specs, out_specs=out_specs, check_vma=False)
```

```python
import functools
import math
import jax
import jax.numpy as jnp
from jax import lax
from jax.experimental import pallas as pl
from jax.experimental.pallas import tpu as pltpu
from jax.sharding import PartitionSpec as P

DEEP_ALPHA = math.sqrt(140.0)
LN_EPS = 1e-5
ROPE_BASE = 10000.0
MESH = pl.DeviceIdType.MESH
CORES = 2
N_VEC = 6
N_LOAD = 1
GROUP = 4
F32 = jnp.float32
BF16 = jnp.bfloat16


def layer_norm(h_val, gain, shift):
    mean_row = jnp.mean(h_val, axis=-1, keepdims=True)
    cent = h_val - mean_row
    var_row = jnp.mean(cent * cent, axis=-1, keepdims=True)
    return (cent * lax.rsqrt(var_row + LN_EPS) * gain + shift).astype(BF16)


def layer_kernel(nx, ny, hid_in, wqkv_in, wo_in, wup_in, wdn_in, bup_in, bqkv_in, pos_in, lens_in, k_in, v_in, *refs):
    vec_in, refs = refs[:N_VEC], refs[N_VEC:]
    out_ref, kc, vc = refs[:3]
    vec_own, refs = refs[3:3 + N_VEC], refs[3 + N_VEC:]
    (hid, wqkv, wo_own, wup_raw, wdn_own, bup, bqkv, pos, lens, qpart, qrecv, qown, kvn, qs, sc, lane,
     wo_far, wup_own, wup_far, wdn_far, vloc, vecs, hid_own, part1, dbuf1, sbuf1, rbuf1, part2, dbuf2, sbuf2, rbuf2,
     zall, obuf, send, recv, load, cache_load) = refs
    nc = ny // CORES
    x, y = lax.axis_index('x'), lax.axis_index('y')
    core, chip = lax.rem(y, CORES), lax.div(y, CORES)
    partner = {'y': chip * CORES + (1 - core)}
    blk = core * nc + chip
    total_slots, heads, dim, all_rows = k_in.shape
    half = dim // 2
    width = hid_in.shape[1]
    own = all_rows // nx
    per = own // ny
    n_out = wqkv_in.shape[1]

    def chip_at(d):
        return lax.rem(chip + d + nc, nc)

    def x_at(d):
        return lax.rem(x + d + nx, nx)

    def chip_dev(d):
        return {'y': chip_at(d) * CORES + core}

    def x_dev(d):
        return {'x': x_at(d)}

    def grid_dev(dx, dc):
        return {'x': x_at(dx), 'y': chip_at(dc) * CORES + core}

    def x_cols(d):
        return pl.ds(pl.multiple_of(x_at(d) * width, width), width)

    def x_rows(d):
        return pl.ds(pl.multiple_of(x_at(d) * own, own), own)

    cols = x_rows(0)
    counter = [0]
    started = []

    def ids(n):
        counter[0] += n
        return list(range(counter[0] - n, counter[0]))

    def copy(src, dst, i, dev):
        return pltpu.make_async_remote_copy(src_ref=src, dst_ref=dst, send_sem=send.at[i], recv_sem=recv.at[i],
                                            device_id=dev, device_id_type=MESH)

    def start(src, dst, i, dev):
        cp = copy(src, dst, i, dev)
        cp.start()
        started.append(cp)

    def arrived(ref, i):
        copy(ref, ref, i, partner).wait_recv()

    pairs = [(hid_in, hid), (wqkv_in, wqkv), (bqkv_in, bqkv), (pos_in, pos), (lens_in, lens), (bup_in, bup),
             (wo_in, wo_own), (wup_in, wup_raw), (wdn_in, wdn_own)] + list(zip(vec_in, vec_own))
    loads = [pltpu.make_async_copy(src, dst, load.at[i]) for i, (src, dst) in enumerate(pairs)]
    for cp in loads:
        cp.start()
    step = total_slots // N_LOAD
    cache_loads = [[pltpu.make_async_copy(src.at[pl.ds(i * step, step)], dst.at[pl.ds(i * step, step)],
                                          cache_load.at[j, i]) for i in range(N_LOAD)]
                   for j, (src, dst) in enumerate(((k_in, kc), (v_in, vc)))]

    barrier = pltpu.get_barrier_semaphore()
    grid = [(dx, dc) for dx in (2, 1, 3, 0) for dc in (2, 1, 3, 0) if dx or dc]
    peers = [partner] + [grid_dev(dx, dc) for dx, dc in grid]
    for dev in peers:
        pl.semaphore_signal(barrier, inc=1, device_id=dev, device_id_type=MESH)
    for cp in loads:
        cp.wait()
    w_t = wqkv[...].T

    def product(d):
        return lax.dot_general(w_t, hid[x_rows(d), :], (((1,), (1,)), ((), ())), preferred_element_type=F32)

    order = [2, 1, 3]
    for d in order:
        qpart[d - 1] = product(d).astype(BF16)
    pl.semaphore_wait(barrier, len(peers))

    q_ids, wo_ids, hid_ids, vec_ids, kv_ids = (ids(nx - 1) for _ in range(5))
    for d in order:
        start(qpart.at[d - 1], qrecv.at[d - 1], q_ids[d - 1], x_dev(d))
    for i in range(N_VEC):
        vloc[i:i + 1, :] = vec_own[i][...].reshape(1, width).astype(F32)

    def my_rows(d):
        return pl.ds(pl.multiple_of(x_at(d) * own + blk * per, per), per)

    for d in order:
        start(wo_own, wo_far.at[d - 1], wo_ids[d - 1], x_dev(d))
        start(hid.at[my_rows(d)], hid_own.at[:, x_cols(0)], hid_ids[d - 1], x_dev(d))
        start(vloc, vecs.at[:, x_cols(0)], vec_ids[d - 1], x_dev(d))

    class Ring:
        def __init__(self, piece, buf):
            self.piece, self.buf = piece, buf
            self.ra, self.rb, self.lb, self.la, self.fa, self.fb = ids(6)

        def begin(self):
            start(self.piece(0), self.buf(2, 0), self.ra, x_dev(1))
            start(self.piece(1), self.buf(0, 1), self.lb, x_dev(-1))

        def rest(self):
            start(self.piece(1), self.buf(2, 1), self.rb, x_dev(1))
            start(self.piece(0), self.buf(0, 0), self.la, x_dev(-1))

        def forward(self):
            arrived(self.buf(2, 0), self.ra)
            start(self.buf(2, 0), self.buf(1, 0), self.fa, x_dev(1))
            arrived(self.buf(0, 1), self.lb)
            start(self.buf(0, 1), self.buf(1, 1), self.fb, x_dev(-1))

        def near(self):
            arrived(self.buf(2, 1), self.rb)
            arrived(self.buf(0, 0), self.la)

        def far(self):
            arrived(self.buf(1, 0), self.fa)
            arrived(self.buf(1, 1), self.fb)

    hd = wdn_own.shape[0] // 2
    up_ring = Ring(lambda h: wup_own.at[h], lambda s, h: wup_far.at[s, h])
    down_ring = Ring(lambda h: wdn_own.at[pl.ds(h * hd, hd)], lambda s, h: wdn_far.at[s, pl.ds(h * hd, hd)])
    for i in range(2):
        wup_own[i] = wup_raw[:, i, :]
    up_ring.begin()
    for group in cache_loads:
        for cp in group:
            cp.start()

    qown[...] = product(0)
    vecs[:, x_cols(0)] = vloc[...]
    hid_own[:, x_cols(0)] = hid[my_rows(0), :]
    freq = jnp.exp(lax.broadcasted_iota(jnp.int32, (half, own), 0).astype(F32) * (-2.0 * math.log(ROPE_BASE) / dim))
    angle = pos[:, cols].astype(F32) * freq
    cos_t, sin_t = jnp.cos(angle), jnp.sin(angle)
    bias = jnp.broadcast_to(bqkv[...].reshape(1, n_out).astype(F32), (128, n_out)).T
    lane[...] = jnp.broadcast_to(lens[...].astype(F32), lane.shape).astype(BF16)

    total = qown[...]
    for d in order:
        arrived(qrecv.at[d - 1], q_ids[d - 1])
        total = total + qrecv[d - 1].astype(F32)
    qkv = (total + bias[:, 0:1]).astype(BF16)

    def rotate(v):
        lo, up = v[:half].astype(F32), v[half:].astype(F32)
        return jnp.concatenate([lo * cos_t - up * sin_t, up * cos_t + lo * sin_t], axis=0).astype(BF16)

    for h in range(heads):
        base = 3 * h * dim
        qs[h] = rotate(qkv[base:base + dim]).astype(F32)
        kvn[0, h, :, cols] = rotate(qkv[base + dim:base + 2 * dim])
        kvn[1, h, :, cols] = qkv[base + 2 * dim:base + 3 * dim]

    def score_step(i, carry):
        for s in range(GROUP):
            for h in range(heads):
                sc[h, pl.ds(i * GROUP + s, 1), :] = jnp.sum(
                    kc[i * GROUP + s, h, :, cols].astype(F32) * qs[h], axis=0, keepdims=True)
        return carry

    for cp in cache_loads[0]:
        cp.wait()
    lax.fori_loop(0, total_slots // GROUP, score_step, 0)
    slot_id = lax.broadcasted_iota(jnp.int32, (total_slots, own), 0)
    own_len = lens[:, cols]
    ok, hit = slot_id <= own_len, slot_id == own_len
    p_new = []
    for h in range(heads):
        s_new = jnp.sum(kvn[0, h, :, cols].astype(F32) * qs[h], axis=0, keepdims=True)
        s = jnp.where(hit, s_new, sc[h]) * (dim ** -0.5)
        s = jnp.where(ok, s, -1e30)
        e = jnp.exp(s - jnp.max(s, axis=0, keepdims=True))
        p = (e / jnp.sum(e, axis=0, keepdims=True)).astype(BF16).astype(F32)
        p_new.append(jnp.sum(jnp.where(hit, p, 0.0), axis=0, keepdims=True))
        sc[h] = jnp.where(hit, 0.0, p)
    for h in range(heads):
        qs[h] = p_new[h] * kvn[1, h, :, cols].astype(F32)

    def mix_step(i, carry):
        for h in range(heads):
            a = qs[h]
            for s in range(GROUP):
                a = a + vc[i * GROUP + s, h, :, cols].astype(F32) * sc[h, pl.ds(i * GROUP + s, 1), :]
            qs[h] = a
        return carry

    for cp in cache_loads[1]:
        cp.wait()
    lax.fori_loop(0, total_slots // GROUP, mix_step, 0)
    attn = qs[...].reshape(heads * dim, own).T.astype(BF16)

    def update(ref, which):
        def write(i, carry):
            for s in range(GROUP):
                slot_hit = lane[...] == (i * GROUP + s).astype(F32).astype(BF16)
                for h in range(heads):
                    for t in range(dim // 16):
                        part = pl.ds(t * 16, 16)
                        ref[i * GROUP + s, h, part, :] = jnp.where(
                            slot_hit, kvn[which, h, part, :], ref[i * GROUP + s, h, part, :])
            return carry

        lax.fori_loop(0, total_slots // GROUP, write, 0)

    def vec(i):
        return vecs[i:i + 1, :]

    def scatter_sum(part, dbuf, sbuf, rbuf, meanwhile):
        base = ids(nc)
        start(part.at[1 - core], dbuf, base[0], partner)
        arrived(dbuf, base[0])
        sbuf[...] = (part[core].astype(F32) + dbuf[...].astype(F32)).astype(BF16)
        for d in (2, 1, 3):
            start(sbuf.at[chip_at(d)], rbuf.at[d - 1], base[d], chip_dev(d))
        meanwhile()
        sums = sbuf[chip].astype(F32)
        for d in range(1, nc):
            arrived(rbuf.at[d - 1], base[d])
            sums = sums + rbuf[d - 1].astype(F32)
        return sums

    def share(buf_at, meanwhile):
        far, near = ids(nc), ids(nc)
        for d in (2, 1, 3):
            start(buf_at(blk), buf_at(blk), far[d], chip_dev(d))
        start(buf_at(blk), buf_at(blk), near[0], partner)
        meanwhile()
        for d in (1, 3, 2):
            ref = buf_at(core * nc + chip_at(-d))
            arrived(ref, far[d])
            start(ref, ref, near[d], partner)
        for d in (0, 1, 3, 2):
            arrived(buf_at((1 - core) * nc + chip_at(-d)), near[d])

    def put(part, d, value):
        part[:, :, :, x_cols(d)] = value.astype(BF16).reshape(CORES, nc, per, width)

    put(part1, 0, jnp.dot(attn, wo_own[...], preferred_element_type=F32))
    for d in order:
        arrived(wo_far.at[d - 1], wo_ids[d - 1])
        put(part1, -d, jnp.dot(attn, wo_far[d - 1], preferred_element_type=F32))
    total = scatter_sum(part1, dbuf1, sbuf1, rbuf1, lambda: (up_ring.rest(), down_ring.begin()))
    for d in range(1, nx):
        arrived(hid_own.at[:, x_cols(-d)], hid_ids[d - 1])
        arrived(vecs.at[:, x_cols(-d)], vec_ids[d - 1])
    h_attn = DEEP_ALPHA * hid_own[...].astype(F32) + total + vec(0)
    zall[blk] = layer_norm(h_attn, vec(1), vec(2))
    def send_weights():
        up_ring.forward()
        down_ring.rest()

    share(lambda b: zall.at[b], send_weights)

    ups = [(0, wup_own), (1, wup_far.at[0]), (-1, wup_far.at[2]), (2, wup_far.at[1])]
    downs = [(0, wdn_own), (1, wdn_far.at[0]), (-1, wdn_far.at[2]), (2, wdn_far.at[1])]
    gate = bup[0:1, :].astype(F32)
    val = bup[1:2, :].astype(F32)
    up_ring.near()
    for d, w in ups:
        if d == 2:
            up_ring.far()
            down_ring.forward()
        zb = zall[:, :, x_cols(d)].reshape(own, width)
        gate = gate + jnp.dot(zb, w[0], preferred_element_type=F32)
        val = val + jnp.dot(zb, w[1], preferred_element_type=F32)
    g = (jax.nn.gelu(gate, approximate=True) * val).astype(BF16)
    down_ring.near()
    for d, w in downs:
        if d == 2:
            down_ring.far()
        put(part2, d, jnp.dot(g, w[...], preferred_element_type=F32))
    def send_kv():
        for d in order:
            own_kv = kvn.at[:, :, :, cols]
            start(own_kv, own_kv, kv_ids[d - 1], x_dev(d))

    total = scatter_sum(part2, dbuf2, sbuf2, rbuf2, send_kv)
    h_mlp = DEEP_ALPHA * zall[blk].astype(F32) + total + vec(3)
    o = layer_norm(h_mlp, vec(4), vec(5))
    for b in range(nx):
        obuf[b] = o[:, b * width:(b + 1) * width]
    out_ids = ids(nx * nc + 1)
    for dx, dc in grid:
        start(obuf.at[x_at(dx)], out_ref.at[x, blk], out_ids[dx * nc + dc], grid_dev(dx, dc))
    out_ref[x, blk] = obuf[x]
    for d in range(1, nx):
        arrived(kvn.at[:, :, :, x_rows(-d)], kv_ids[d - 1])
    update(kc, 0)
    update(vc, 1)
    for dx, dc in grid:
        arrived(out_ref.at[x_at(-dx), core * nc + chip_at(-dc)], out_ids[dx * nc + dc])
    mine = out_ref.at[:, pl.ds(core * nc, nc)]
    start(mine, mine, out_ids[nx * nc], partner)
    arrived(out_ref.at[:, pl.ds((1 - core) * nc, nc)], out_ids[nx * nc])
    for cp in started:
        cp.wait_send()


def layer(nx, ny, hidden, w_qkv, w_out, w_up, w_down, b_up, b_qkv, positions, lengths, k_t, v_t, vecs):
    nc = ny // CORES
    rows, width = hidden.shape
    total_slots, heads, dim, _ = k_t.shape
    own = rows // nx
    per = own // ny
    total_width = width * nx
    n_out = w_qkv.shape[1]
    up_shape = (w_up.shape[1], w_up.shape[0], w_up.shape[2])
    n_sem = 5 * (nx - 1) + 12 + 4 * nc + nx * nc + 1
    hbm = pl.BlockSpec(memory_space=pltpu.HBM)
    vm = pl.BlockSpec(memory_space=pltpu.VMEM)
    reduce_bufs = [pltpu.VMEM((CORES, nc, per, total_width), BF16), pltpu.VMEM((nc, per, total_width), BF16),
                   pltpu.VMEM((nc, per, total_width), BF16), pltpu.VMEM((nc - 1, per, total_width), BF16)]
    ins = (hidden, w_qkv, w_out, w_up, w_down, b_up, b_qkv, positions.reshape(1, rows), lengths.reshape(1, rows))
    out, k_t, v_t = pl.pallas_call(
        functools.partial(layer_kernel, nx, ny),
        out_shape=(jax.ShapeDtypeStruct((nx, ny, per, width), BF16), pltpu.VMEM(k_t.shape, BF16),
                   pltpu.VMEM(v_t.shape, BF16)),
        in_specs=[hbm] * (len(ins) + 2 + N_VEC),
        out_specs=(vm,) * 3,
        scratch_shapes=[pltpu.VMEM(v.shape, BF16) for v in vecs] + [
            pltpu.VMEM(a.shape, a.dtype) for a in (hidden, w_qkv, w_out, w_up, w_down, b_up, b_qkv, ins[7], ins[8])] + [
            pltpu.VMEM((nx - 1, n_out, own), BF16), pltpu.VMEM((nx - 1, n_out, own), BF16),
            pltpu.VMEM((n_out, own), F32), pltpu.VMEM((2, heads, dim, rows), BF16),
            pltpu.VMEM((heads, dim, own), F32), pltpu.VMEM((heads, total_slots, own), F32),
            pltpu.VMEM((16, rows), BF16), pltpu.VMEM((nx - 1,) + w_out.shape, BF16),
            pltpu.VMEM(up_shape, BF16), pltpu.VMEM((nx - 1,) + up_shape, BF16), pltpu.VMEM((nx - 1,) + w_down.shape, BF16),
            pltpu.VMEM((8, width), F32), pltpu.VMEM((8, total_width), F32), pltpu.VMEM((per, total_width), BF16),
        ] + reduce_bufs + reduce_bufs + [
            pltpu.VMEM((ny, per, total_width), BF16), pltpu.VMEM((nx, per, width), BF16),
            pltpu.SemaphoreType.DMA((n_sem,)), pltpu.SemaphoreType.DMA((n_sem,)),
            pltpu.SemaphoreType.DMA((len(ins) + N_VEC,)), pltpu.SemaphoreType.DMA((2, N_LOAD))],
        compiler_params=pltpu.CompilerParams(collective_id=0, has_side_effects=True, vmem_limit_bytes=24 * 2**20),
        name='layer',
    )(*ins, k_t, v_t, *vecs)
    return out.reshape(rows, width), k_t, v_t


def solution(mesh):
    nx, ny = mesh.shape['x'], mesh.shape['y']
    cache_spec = P('dp', None, 'y', None)
    width_spec = P('x')
    in_specs = (P('dp', 'x'), P('x', 'y'), P('y'), P('y', 'x'), width_spec, width_spec, width_spec, P('x', None, 'y'), P(None, 'y'), P('y', 'x'), width_spec, width_spec, width_spec, cache_spec, cache_spec, P('dp'), P('dp'))
    out_specs = (P('dp', 'x'), cache_spec, cache_spec)

    def local_step(hidden, w_qkv, b_qkv, w_out, b_out, attn_gain, attn_shift, w_up, b_up, w_down, b_down, mlp_gain, mlp_shift, k_cache, v_cache, positions, lengths):
        k_t, v_t = jnp.transpose(k_cache, (1, 2, 3, 0)), jnp.transpose(v_cache, (1, 2, 3, 0))
        vecs = (b_out, attn_gain, attn_shift, b_down, mlp_gain, mlp_shift)
        result, k_t, v_t = layer(nx, ny, hidden, w_qkv, w_out, w_up, w_down, b_up, b_qkv, positions, lengths, k_t, v_t, vecs)
        k_full, v_full = jnp.transpose(k_t, (3, 0, 1, 2)), jnp.transpose(v_t, (3, 0, 1, 2))
        return result, k_full, v_full

    return jax.shard_map(local_step, mesh=mesh, in_specs=in_specs, out_specs=out_specs, check_vma=False)
```
